64 devices in a mesh: dp: 4 (over x, y), sp: 16 (over z, core).
Axes of the slice: x: 2, y: 2, z: 8, core: 2. Of those that a mesh axis runs over, the one named last changes fastest.
The devices are a block of a 4x4x8 slice.
Arguments:
- hidden: bfloat16 [1024, 4096], P(('dp', 'sp')), parts along dimension 0
- w_q: bfloat16 [4096, 12288], replicated
- w_k: bfloat16 [4096, 1024], replicated
- w_v: bfloat16 [4096, 1024], replicated
- w_o: bfloat16 [12288, 4096], replicated
- expert_ids: int32 [1024, 2], P(('dp', 'sp')), parts along dimension 0
- router_probs: float32 [1024, 128], P(('dp', 'sp')), parts along dimension 0
Outputs:
- output 1: bfloat16 [1024, 4096], P(('dp', 'sp')), parts along dimension 0
- output 2: bfloat16 [512, 256, 4096], P(('dp', 'sp')), parts along dimension 0
There are 4 independent parts. The reference program is written for one: setup_inputs(seed, part) draws one part's arguments, and reference() takes and returns one part's arrays. A program takes and returns all parts, laid end to end along the dimension named above; an argument that names none is the same for every part.
All inputs are finite; a program needn't handle non-finite values.
Results may differ from the reference program's by a relative error of at most 0.00852087.
Values are sent between devices in bfloat16 or wider.
A program may use at most 768 MiB of HBM per device.

```python
import math
import jax
import jax.numpy as jnp
from jax import lax

D = 4096
HEADS = 96
KV_HEADS = 8
HEAD = 128
EXPERTS = 128
TOKENS_DEV = 16
GROUP = 16

SEQ = TOKENS_DEV * GROUP
Q_PER_KV = HEADS // KV_HEADS
Q_WIDTH = HEADS * HEAD
KV_WIDTH = KV_HEADS * HEAD
SCORE_SCALE = 1.0 / math.sqrt(HEAD)


def draw_routes(route_key):
    key_first, key_second, key_pick, key_cold, key_order = jax.random.split(route_key, 5)
    hot_first = jax.random.randint(key_first, (), 0, EXPERTS)
    hot_second = (hot_first + 1 + jax.random.randint(key_second, (), 0, EXPERTS - 1)) % EXPERTS
    pick_hot = jax.random.randint(key_pick, (SEQ,), 0, 2)
    cold_ids = (hot_first + 1 + jax.random.randint(key_cold, (SEQ,), 0, EXPERTS - 1)) % EXPERTS
    other_ids = jnp.where(pick_hot == 1, hot_second, cold_ids)
    first_ids = jnp.full((SEQ,), hot_first)
    swap_bits = jax.random.randint(key_order, (SEQ,), 0, 2)
    col_zero = jnp.where(swap_bits == 1, other_ids, first_ids)
    col_one = jnp.where(swap_bits == 1, first_ids, other_ids)
    return jnp.stack([col_zero, col_one], axis=1).astype(jnp.int32)


def setup_inputs(seed: int = 0, part: int = 0) -> dict:
    base_key = jax.random.key(seed)
    part_key = jax.random.fold_in(base_key, part)
    weight_keys = jax.random.split(base_key, 4)
    part_keys = jax.random.split(part_key, 3)
    q_gain = math.sqrt(0.5 * math.log(SEQ))
    o_gain = 0.5 * SEQ ** 0.25
    hidden = jax.random.normal(part_keys[0], (SEQ, D), jnp.float32).astype(jnp.bfloat16)
    w_q = (jax.random.normal(weight_keys[0], (D, Q_WIDTH), jnp.float32) * (q_gain / math.sqrt(D))).astype(jnp.bfloat16)
    w_k = (jax.random.normal(weight_keys[1], (D, KV_WIDTH), jnp.float32) / math.sqrt(D)).astype(jnp.bfloat16)
    w_v = (jax.random.normal(weight_keys[2], (D, KV_WIDTH), jnp.float32) / math.sqrt(D)).astype(jnp.bfloat16)
    w_o = (jax.random.normal(weight_keys[3], (Q_WIDTH, D), jnp.float32) * (o_gain / math.sqrt(Q_WIDTH))).astype(jnp.bfloat16)
    expert_ids = draw_routes(part_keys[1])
    router_probs = jax.nn.softmax(1.5 * jax.random.normal(part_keys[2], (SEQ, EXPERTS), jnp.float32), axis=1)
    return {'hidden': hidden, 'w_q': w_q, 'w_k': w_k, 'w_v': w_v, 'w_o': w_o, 'expert_ids': expert_ids, 'router_probs': router_probs}


def reference(hidden, w_q, w_k, w_v, w_o, expert_ids, router_probs):
    q_all = jnp.dot(hidden, w_q, preferred_element_type=jnp.float32).astype(jnp.bfloat16)
    k_all = jnp.dot(hidden, w_k, preferred_element_type=jnp.float32).astype(jnp.bfloat16)
    v_all = jnp.dot(hidden, w_v, preferred_element_type=jnp.float32).astype(jnp.bfloat16)
    q_groups = q_all.reshape(SEQ, KV_HEADS, Q_PER_KV, HEAD).transpose(1, 0, 2, 3)
    k_groups = k_all.reshape(SEQ, KV_HEADS, HEAD).transpose(1, 0, 2)
    v_groups = v_all.reshape(SEQ, KV_HEADS, HEAD).transpose(1, 0, 2)
    positions = jnp.arange(SEQ)
    causal = positions[:, None] >= positions[None, :]

    def one_group(group_in):
        q_grp, k_grp, v_grp = group_in
        scores = jnp.einsum('qmd,kd->mqk', q_grp.astype(jnp.float32), k_grp.astype(jnp.float32)) * SCORE_SCALE
        scores = jnp.where(causal[None, :, :], scores, -1e30)
        weights = jax.nn.softmax(scores, axis=-1).astype(jnp.bfloat16)
        out_grp = jnp.einsum('mqk,kd->qmd', weights.astype(jnp.float32), v_grp.astype(jnp.float32))
        return out_grp.astype(jnp.bfloat16)

    attn_out = lax.map(one_group, (q_groups, k_groups, v_groups))
    attn_out = attn_out.transpose(1, 0, 2, 3).reshape(SEQ, Q_WIDTH)
    out_proj = jnp.dot(attn_out, w_o, preferred_element_type=jnp.float32)
    hidden_out = (hidden.astype(jnp.float32) + out_proj).astype(jnp.bfloat16)
    picked = jnp.take_along_axis(router_probs, expert_ids, axis=1)
    gate_w = picked / jnp.sum(picked, axis=1, keepdims=True)
    gated = (gate_w[:, :, None] * hidden_out.astype(jnp.float32)[:, None, :]).astype(jnp.bfloat16)
    ids_blk = expert_ids.reshape(GROUP, TOKENS_DEV, 2)
    token_hits = jnp.sum((ids_blk[:, :, :, None] == jnp.arange(EXPERTS)).astype(jnp.int32), axis=2)
    earlier = jnp.cumsum(token_hits, axis=1) - token_hits
    slot_rank = jnp.take_along_axis(earlier, ids_blk, axis=2)
    dest_rows = jnp.arange(GROUP)[:, None, None] * TOKENS_DEV + slot_rank
    buffer = jnp.zeros((EXPERTS, GROUP * TOKENS_DEV, D), jnp.bfloat16)
    buffer = buffer.at[ids_blk, dest_rows].set(gated.reshape(GROUP, TOKENS_DEV, 2, D))
    return (hidden_out, buffer)
```

```python
import math
import functools
import jax
import jax.numpy as jnp
from jax import lax
from jax.experimental import pallas as pl
from jax.experimental.pallas import tpu as pltpu
from jax.sharding import PartitionSpec as P

HEAD_DIM = 128
SCORE_SCALE = 1.0 / math.sqrt(HEAD_DIM)
COLS = 256


def route_table(me, ids, probs, seq, table_rows):
    tok_dev, experts = probs.shape
    lanes = experts
    per_row = lanes // tok_dev
    sub = lax.broadcasted_iota(jnp.int32, (tok_dev, lanes), 0)
    lane = lax.broadcasted_iota(jnp.int32, (tok_dev, lanes), 1)
    tok = lane - tok_dev * lax.rem(me, per_row)
    diag = tok == sub
    e_sub = [ids[:, k:k + 1] for k in range(2)]
    p_sub = [jnp.sum(jnp.where(lane == e, probs, 0.0), axis=1, keepdims=True) for e in e_sub]
    total = p_sub[0] + p_sub[1]
    to_lanes = lambda col: jnp.sum(jnp.where(diag, col, 0.0), axis=0, keepdims=True)
    e_subf = [e.astype(jnp.float32) for e in e_sub]
    e_lane = [to_lanes(e) for e in e_subf]
    valid = jnp.sum(jnp.where(diag, 1.0, 0.0), axis=0, keepdims=True)
    base = (tok_dev * me).astype(jnp.float32)
    dests, gates = [], []
    for k in range(2):
        same = ((e_subf[0] == e_lane[k]) | (e_subf[1] == e_lane[k])) & (sub < tok)
        slot = jnp.sum(jnp.where(same, 1.0, 0.0), axis=0, keepdims=True)
        dests.append(valid * (e_lane[k] * float(seq) + base + slot))
        gates.append(to_lanes(p_sub[k] / total))
    row = lax.broadcasted_iota(jnp.int32, (table_rows, lanes), 0)
    mine = lax.div(me, per_row)
    n_rows = table_rows // 4
    table = jnp.zeros((table_rows, lanes), jnp.float32)
    for n, vec in enumerate(dests + gates):
        table = jnp.where(row == n * n_rows + mine, vec, table)
    return table


def build_kernel(n_chips, h_ref, table_ref, out_ref, hid_ref):
    step = pl.program_id(0)
    me = lax.axis_index('sp')
    experts_dev = pl.num_programs(0)
    n_cols, tok_chip, cols = h_ref.shape[1], h_ref.shape[2], h_ref.shape[3]
    seq = n_chips * tok_chip
    n_rows = table_ref.shape[0] // 4
    table = table_ref[...]
    spread = lambda n: jnp.concatenate([table[n * n_rows + r:n * n_rows + r + 1, :] for r in range(n_rows)], axis=1)
    dest = [spread(0), spread(1)]
    gate = [spread(2), spread(3)]
    expert = me * experts_dev + step

    @pl.when(step == 0)
    def _():
        tok_dev = hid_ref.shape[0]
        per_chip = tok_chip // tok_dev
        chip = lax.div(me, per_chip)
        first = pl.multiple_of(lax.rem(me, per_chip) * tok_dev, tok_dev)
        for n in range(n_cols):
            hid_ref[:, n * cols:(n + 1) * cols] = h_ref[chip, n, pl.ds(first, tok_dev), :]

    row = (lax.broadcasted_iota(jnp.int32, (seq, seq), 0) + expert * seq).astype(jnp.float32)
    hit = [dest[0] == row, dest[1] == row]
    gate_row = jnp.sum(jnp.where(hit[0], gate[0], 0.0) + jnp.where(hit[1], gate[1], 0.0), axis=1, keepdims=True)
    picks = jnp.where(hit[0] | hit[1], 1.0, 0.0)
    any_row = jnp.sum(picks) > 0.0

    @pl.when(any_row)
    def _():
        pick = picks.astype(jnp.bfloat16)
        for n in range(n_cols):
            rows = h_ref[:, n].reshape(seq, cols)
            got = jnp.dot(pick, rows, preferred_element_type=jnp.float32)
            out_ref[0, :, n * cols:(n + 1) * cols] = (got * gate_row).astype(jnp.bfloat16)

    @pl.when(jnp.logical_not(any_row))
    def _():
        out_ref[...] = jnp.zeros_like(out_ref)


def build_buffers(h_all, table, tok_dev, experts_dev):
    n_chips, n_cols, tok_chip, cols = h_all.shape
    seq, width = n_chips * tok_chip, n_cols * cols
    return pl.pallas_call(
        functools.partial(build_kernel, n_chips),
        name='build_buffers',
        grid=(experts_dev,),
        in_specs=[pl.BlockSpec(h_all.shape, lambda e: (0, 0, 0, 0)), pl.BlockSpec(table.shape, lambda e: (0, 0))],
        out_specs=[pl.BlockSpec((1, seq, width), lambda e: (e, 0, 0)), pl.BlockSpec((tok_dev, width), lambda e: (0, 0))],
        out_shape=[jax.ShapeDtypeStruct((experts_dev, seq, width), jnp.bfloat16), jax.ShapeDtypeStruct((tok_dev, width), jnp.bfloat16)],
        compiler_params=pltpu.CompilerParams(vmem_limit_bytes=32 * 1024 * 1024),
        cost_estimate=pl.CostEstimate(flops=2 * experts_dev * seq * seq * width, bytes_accessed=2 * experts_dev * seq * width, transcendentals=0),
    )(h_all, table)


def solution(mesh):
    group = mesh.shape['sp']
    row_spec = P(('dp', 'sp'), None)
    buf_spec = P(('dp', 'sp'), None, None)

    def device_step(x_loc, w_q, w_k, w_v, w_o, ids_loc, probs_loc):
        tok_dev, width = x_loc.shape
        seq_len = tok_dev * group
        n_heads = w_q.shape[1] // HEAD_DIM
        kv_heads = w_k.shape[1] // HEAD_DIM
        kv_copies = max(1, group // kv_heads)
        head_dev = n_heads // group
        kv_dev = kv_heads * kv_copies // group
        q_loc = jnp.dot(x_loc, w_q, preferred_element_type=jnp.float32).astype(jnp.bfloat16).reshape(tok_dev, n_heads, HEAD_DIM)
        k_loc = jnp.dot(x_loc, w_k, preferred_element_type=jnp.float32).astype(jnp.bfloat16).reshape(tok_dev, kv_heads, HEAD_DIM)
        v_loc = jnp.dot(x_loc, w_v, preferred_element_type=jnp.float32).astype(jnp.bfloat16).reshape(tok_dev, kv_heads, HEAD_DIM)
        k_loc = jnp.repeat(k_loc, kv_copies, axis=1)
        v_loc = jnp.repeat(v_loc, kv_copies, axis=1)
        q_seq = lax.all_to_all(q_loc, 'sp', 1, 0, tiled=True)
        k_seq = lax.all_to_all(k_loc, 'sp', 1, 0, tiled=True)
        v_seq = lax.all_to_all(v_loc, 'sp', 1, 0, tiled=True)
        q_grp = q_seq.reshape(seq_len, kv_dev, head_dev // kv_dev, HEAD_DIM)
        scores = jnp.einsum('qgmd,kgd->gmqk', q_grp, k_seq, preferred_element_type=jnp.float32) * SCORE_SCALE
        positions = jnp.arange(seq_len)
        causal = positions[:, None] >= positions[None, :]
        weights = jax.nn.softmax(jnp.where(causal, scores, -1e30), axis=-1).astype(jnp.bfloat16)
        attn_seq = jnp.einsum('gmqk,kgd->qgmd', weights, v_seq, preferred_element_type=jnp.float32).astype(jnp.bfloat16)
        attn_seq = attn_seq.reshape(seq_len, head_dev, HEAD_DIM)
        attn_loc = lax.all_to_all(attn_seq, 'sp', 0, 1, tiled=True).reshape(tok_dev, n_heads * HEAD_DIM)
        out_proj = jnp.dot(attn_loc, w_o, preferred_element_type=jnp.float32)
        hidden_out = (x_loc.astype(jnp.float32) + out_proj).astype(jnp.bfloat16)
        experts_dev = probs_loc.shape[1] // group
        table = route_table(lax.axis_index('sp'), ids_loc, probs_loc, seq_len, 4 * seq_len // probs_loc.shape[1])
        table = jnp.sum(lax.all_gather(table, 'sp', axis=0), axis=0)
        h_all = lax.all_gather(hidden_out, 'sp', axis=0, tiled=True)
        h_all = h_all.reshape(group // 2, 2 * tok_dev, width // COLS, COLS).transpose(0, 2, 1, 3)
        buf, hid = build_buffers(h_all, table, tok_dev, experts_dev)
        return hid, buf

    return jax.shard_map(device_step, mesh=mesh, in_specs=(row_spec, P(), P(), P(), P(), row_spec, row_spec), out_specs=(row_spec, buf_spec), check_vma=False)
```

```python
import math
import functools
import jax
import jax.numpy as jnp
from jax import lax
from jax.experimental import pallas as pl
from jax.experimental.pallas import tpu as pltpu
from jax.sharding import PartitionSpec as P

HEAD_DIM = 128
SCORE_SCALE = 1.0 / math.sqrt(HEAD_DIM)
COLS = 256


def route_table(me, ids, probs, seq, table_rows):
    tok_dev, experts = probs.shape
    lanes = experts
    per_row = lanes // tok_dev
    sub = lax.broadcasted_iota(jnp.int32, (tok_dev, lanes), 0)
    lane = lax.broadcasted_iota(jnp.int32, (tok_dev, lanes), 1)
    tok = lane - tok_dev * lax.rem(me, per_row)
    diag = tok == sub
    e_sub = [ids[:, k:k + 1] for k in range(2)]
    p_sub = [jnp.sum(jnp.where(lane == e, probs, 0.0), axis=1, keepdims=True) for e in e_sub]
    total = p_sub[0] + p_sub[1]
    to_lanes = lambda col: jnp.sum(jnp.where(diag, col, 0.0), axis=0, keepdims=True)
    e_subf = [e.astype(jnp.float32) for e in e_sub]
    e_lane = [to_lanes(e) for e in e_subf]
    valid = jnp.sum(jnp.where(diag, 1.0, 0.0), axis=0, keepdims=True)
    base = (tok_dev * me).astype(jnp.float32)
    dests, gates = [], []
    for k in range(2):
        same = ((e_subf[0] == e_lane[k]) | (e_subf[1] == e_lane[k])) & (sub < tok)
        slot = jnp.sum(jnp.where(same, 1.0, 0.0), axis=0, keepdims=True)
        dests.append(valid * (e_lane[k] * float(seq) + base + slot))
        gates.append(to_lanes(p_sub[k] / total))
    row = lax.broadcasted_iota(jnp.int32, (table_rows, lanes), 0)
    mine = lax.div(me, per_row)
    n_rows = table_rows // 4
    table = jnp.zeros((table_rows, lanes), jnp.float32)
    for n, vec in enumerate(dests + gates):
        table = jnp.where(row == n * n_rows + mine, vec, table)
    return table


def build_kernel(n_chips, h_ref, table_ref, out_ref, hid_ref):
    step = pl.program_id(0)
    me = lax.axis_index('sp')
    experts_dev = pl.num_programs(0)
    n_cols, tok_chip, cols = h_ref.shape[1], h_ref.shape[2], h_ref.shape[3]
    seq = n_chips * tok_chip
    n_rows = table_ref.shape[0] // 4
    table = table_ref[...]
    spread = lambda n: jnp.concatenate([table[n * n_rows + r:n * n_rows + r + 1, :] for r in range(n_rows)], axis=1)
    dest = [spread(0), spread(1)]
    gate = [spread(2), spread(3)]
    expert = me * experts_dev + step

    @pl.when(step == 0)
    def _():
        tok_dev = hid_ref.shape[0]
        per_chip = tok_chip // tok_dev
        chip = lax.div(me, per_chip)
        first = pl.multiple_of(lax.rem(me, per_chip) * tok_dev, tok_dev)
        for n in range(n_cols):
            hid_ref[:, n * cols:(n + 1) * cols] = h_ref[chip, n, pl.ds(first, tok_dev), :]

    row = (lax.broadcasted_iota(jnp.int32, (seq, seq), 0) + expert * seq).astype(jnp.float32)
    hit = [dest[0] == row, dest[1] == row]
    gate_row = jnp.sum(jnp.where(hit[0], gate[0], 0.0) + jnp.where(hit[1], gate[1], 0.0), axis=1, keepdims=True)
    picks = jnp.where(hit[0] | hit[1], 1.0, 0.0)
    any_row = jnp.sum(picks) > 0.0

    @pl.when(any_row)
    def _():
        pick = picks.astype(jnp.bfloat16)
        for n in range(n_cols):
            rows = h_ref[:, n].reshape(seq, cols)
            got = jnp.dot(pick, rows, preferred_element_type=jnp.float32)
            out_ref[0, :, n * cols:(n + 1) * cols] = (got * gate_row).astype(jnp.bfloat16)

    @pl.when(jnp.logical_not(any_row))
    def _():
        out_ref[...] = jnp.zeros_like(out_ref)


def build_buffers(h_all, table, tok_dev, experts_dev):
    n_chips, n_cols, tok_chip, cols = h_all.shape
    seq, width = n_chips * tok_chip, n_cols * cols
    return pl.pallas_call(
        functools.partial(build_kernel, n_chips),
        name='build_buffers',
        grid=(experts_dev,),
        in_specs=[pl.BlockSpec(h_all.shape, lambda e: (0, 0, 0, 0)), pl.BlockSpec(table.shape, lambda e: (0, 0))],
        out_specs=[pl.BlockSpec((1, seq, width), lambda e: (e, 0, 0)), pl.BlockSpec((tok_dev, width), lambda e: (0, 0))],
        out_shape=[jax.ShapeDtypeStruct((experts_dev, seq, width), jnp.bfloat16), jax.ShapeDtypeStruct((tok_dev, width), jnp.bfloat16)],
        compiler_params=pltpu.CompilerParams(vmem_limit_bytes=32 * 1024 * 1024),
        cost_estimate=pl.CostEstimate(flops=2 * experts_dev * seq * seq * width, bytes_accessed=2 * experts_dev * seq * width, transcendentals=0),
    )(h_all, table)


MESH = pl.DeviceIdType.MESH
ROWS = 2048
LAG = 2


def block_kernel(group, x_hbm, wq, wk, wv, wo, ids, probs, h_out, table_out, wbuf, x_buf, kv, q_buf, o_buf, h_all, tab_pair, tabs,
                 w_sem, x_sem, pair_send, pair_recv, kv_send, kv_recv, tab_send, tab_recv, o_send, o_recv,
                 h_send, h_recv, d_send, d_recv, out_sem):
    tok_dev, width = x_hbm.shape
    chips = kv.shape[0]
    tok_chip = x_buf.shape[0]
    seq = chips * tok_chip
    heads_core = q_buf.shape[0]
    kv_core = kv.shape[3] // HEAD_DIM
    per_kv = heads_core // kv_core
    q_core = heads_core * HEAD_DIM
    out_core = width // 2
    me = lax.axis_index('sp')
    chip, core = lax.div(me, 2), lax.rem(me, 2)
    other = 1 - core
    partner = {'sp': 2 * chip + other}
    ahead = {'sp': 2 * lax.rem(chip + 1, chips) + core}
    behind = {'sp': 2 * lax.rem(chip + chips - 1, chips) + core}

    def remote(src, dst, send, recv, device):
        return pltpu.make_async_remote_copy(src_ref=src, dst_ref=dst, send_sem=send, recv_sem=recv, device_id=device, device_id_type=MESH)

    n_slots = wbuf.shape[0]
    kv_units = 2 * (kv.shape[3] // COLS) * (width // ROWS)
    half_units = q_core // ROWS
    chunk_units = 2 * half_units
    in_units = width // ROWS
    q_chunks = q_core // COLS
    o_chunks = out_core // COLS
    kv_chunks = kv.shape[3] // COLS

    def load(src, row, col, slot):
        return pltpu.make_async_copy(src.at[pl.ds(row, ROWS), pl.ds(pl.multiple_of(col, COLS), COLS)], wbuf.at[slot], w_sem.at[slot])

    def wait_unit(slot):
        load(wk, 0, 0, slot).wait()

    def start_q(n):
        for r in range(in_units):
            load(wq, r * ROWS, core * q_core + n * COLS, lax.rem(kv_units + in_units * n + r, n_slots)).start()

    first_o = kv_units + in_units * q_chunks - n_slots

    def start_o(k):
        j, r = lax.div(k, chunk_units), lax.rem(k, chunk_units)
        half = jnp.where(r < half_units, core, other)
        row = pl.multiple_of(half * q_core + lax.rem(r, half_units) * ROWS, ROWS)
        load(wo, row, core * out_core + j * COLS, first_o + k).start()

    own = pl.ds(pl.multiple_of(core * tok_dev, tok_dev), tok_dev)
    x_in = pltpu.make_async_copy(x_hbm, x_buf.at[own], x_sem)
    x_in.start()
    slot = 0
    for src in (wk, wv):
        for n in range(kv_chunks):
            for r in range(in_units):
                load(src, r * ROWS, core * kv.shape[3] + n * COLS, slot).start()
                slot += 1
    q_first = (n_slots - kv_units) // in_units
    lax.fori_loop(0, q_first, lambda n, c: (start_q(n), c)[1], 0)

    barrier = pltpu.get_barrier_semaphore()
    for device in (partner, ahead, behind):
        pl.semaphore_signal(barrier, inc=1, device_id=device, device_id_type=MESH)
    tab_pair[0] = route_table(me, ids[...], probs[...], seq, tab_pair.shape[1])
    x_in.wait()
    pl.semaphore_wait(barrier, 3)

    x_pair = remote(x_buf.at[own], x_buf.at[own], pair_send.at[0], pair_recv.at[0], partner)
    t_pair = remote(tab_pair.at[0], tab_pair.at[1], pair_send.at[1], pair_recv.at[1], partner)
    x_pair.start()
    t_pair.start()
    theirs = pl.ds(pl.multiple_of(other * tok_dev, tok_dev), tok_dev)
    remote(x_buf.at[theirs], x_buf.at[theirs], pair_send.at[0], pair_recv.at[0], partner).wait_recv()
    t_pair.wait_recv()
    tabs[chip] = tab_pair[0] + tab_pair[1]

    def project(pair_slot):
        for r in range(in_units):
            wait_unit(pair_slot + r)
        w = wbuf[pl.ds(pair_slot, in_units)].reshape(width, COLS)
        return jnp.dot(x_buf[...], w, preferred_element_type=jnp.float32).astype(jnp.bfloat16)

    slot = 0
    for which in range(2):
        for n in range(kv_chunks):
            kv[chip, which, :, n * COLS:(n + 1) * COLS] = project(slot)
            slot += in_units

    for n in range(q_first, q_chunks):
        start_q(n)
    early = kv_units - first_o
    for k in range(early):
        start_o(k)

    def ring(buf, sends, recvs, s, back):
        block = lax.rem(chip + s, chips) if back else lax.rem(chip + chips - s, chips)
        n = 4 * back + s
        return remote(buf.at[block], buf.at[block], sends.at[n], recvs.at[n], behind if back else ahead)

    def ring_in(buf, sends, recvs, s, back):
        block = lax.rem(chip + s + 1, chips) if back else lax.rem(chip + chips - s - 1, chips)
        n = 4 * back + s
        return remote(buf.at[block], buf.at[block], sends.at[n], recvs.at[n], behind if back else ahead)

    small = ((kv, kv_send, kv_recv), (tabs, tab_send, tab_recv))
    fwd, bwd = chips // 2, chips // 2 - 1
    for args in small:
        ring(*args, 0, 0).start()
        ring(*args, 0, 1).start()

    heads_chunk = COLS // HEAD_DIM

    def q_step(n, carry):
        res = project(lax.rem(kv_units + in_units * n, n_slots))
        for i in range(heads_chunk):
            q_buf[heads_chunk * n + i] = res[:, i * HEAD_DIM:(i + 1) * HEAD_DIM]

        @pl.when(n < q_first)
        def _():
            for r in range(in_units):
                start_o(early + in_units * n + r)
        return carry

    part = q_chunks // fwd
    for s in range(fwd):
        lax.fori_loop(s * part, (s + 1) * part, q_step, 0)
        for args in small:
            ring_in(*args, s, 0).wait_recv()
            if s + 1 < fwd:
                ring(*args, s + 1, 0).start()
            if s < bwd:
                ring_in(*args, s, 1).wait_recv()
                if s + 1 < bwd:
                    ring(*args, s + 1, 1).start()

    rows = per_kv * tok_chip
    q_pos = tok_chip * chip + lax.rem(lax.broadcasted_iota(jnp.int32, (rows, seq), 0), tok_chip)
    seen = lax.broadcasted_iota(jnp.int32, (rows, seq), 1) <= q_pos
    o_copies = []
    for g in range(kv_core):
        lanes = slice(g * HEAD_DIM, (g + 1) * HEAD_DIM)
        qg = q_buf[g * per_kv:(g + 1) * per_kv].reshape(rows, HEAD_DIM)
        kg = kv[:, 0, :, lanes].reshape(seq, HEAD_DIM)
        vg = kv[:, 1, :, lanes].reshape(seq, HEAD_DIM)
        s = lax.dot_general(qg, kg, (((1,), (1,)), ((), ())), preferred_element_type=jnp.float32) * SCORE_SCALE
        s = jnp.where(seen, s, -1e30)
        p = jnp.exp(s - jnp.max(s, axis=1, keepdims=True))
        p = (p / jnp.sum(p, axis=1, keepdims=True)).astype(jnp.bfloat16)
        o = jnp.dot(p, vg, preferred_element_type=jnp.float32).astype(jnp.bfloat16)
        for h in range(per_kv):
            at = (g * per_kv + h) * HEAD_DIM
            o_buf[0, :, at:at + HEAD_DIM] = o[h * tok_chip:(h + 1) * tok_chip]
        span = pl.ds(g * per_kv * HEAD_DIM, per_kv * HEAD_DIM)
        copy = remote(o_buf.at[0, :, span], o_buf.at[1, :, span], o_send.at[g], o_recv.at[g], partner)
        copy.start()
        o_copies.append(copy)

    def h_piece(block, j, s, back):
        piece = h_all.at[block, core * o_chunks + j]
        if s == fwd - 1:
            piece = piece.at[pl.ds(back * tok_dev, tok_dev)]
        return piece

    def h_ring(j, s, back):
        block = lax.rem(chip + s, chips) if back else lax.rem(chip + chips - s, chips)
        piece = h_piece(block, j, s, back)
        return remote(piece, piece, h_send.at[j, 4 * back + s], h_recv.at[j, 4 * back + s], behind if back else ahead)

    def h_ring_in(j, s, back):
        block = lax.rem(chip + s + 1, chips) if back else lax.rem(chip + chips - s - 1, chips)
        piece = h_piece(block, j, s, back)
        return remote(piece, piece, h_send.at[j, 4 * back + s], h_recv.at[j, 4 * back + s], behind if back else ahead)

    def h_pair(j):
        cols = h_all.at[:, core * o_chunks + j]
        return remote(cols, cols, d_send.at[j], d_recv.at[j], partner)

    def h_pair_in(j):
        cols = h_all.at[:, other * o_chunks + j]
        return remote(cols, cols, d_send.at[j], d_recv.at[j], partner)

    def h_hop(j, s):
        for back in range(2):
            h_ring_in(j, s, back).wait_recv()
            if s + 1 < fwd:
                h_ring(j, s + 1, back).start()
        if s + 1 == fwd:
            h_pair(j).start()

    def o_step(j, carry):
        at = first_o + chunk_units * j
        for r in range(half_units):
            wait_unit(at + r)
        acc = jnp.dot(o_buf[0], wbuf[pl.ds(at, half_units)].reshape(q_core, COLS), preferred_element_type=jnp.float32)

        @pl.when(j == 0)
        def _():
            for copy in o_copies:
                copy.wait_recv()
        for r in range(half_units):
            wait_unit(at + half_units + r)
        acc += jnp.dot(o_buf[1], wbuf[pl.ds(at + half_units, half_units)].reshape(q_core, COLS), preferred_element_type=jnp.float32)
        x_cols = x_buf[:, pl.ds(pl.multiple_of(core * out_core + j * COLS, COLS), COLS)]
        h_all[chip, core * o_chunks + j] = (x_cols.astype(jnp.float32) + acc).astype(jnp.bfloat16)
        for back in range(2):
            h_ring(j, 0, back).start()
        for s in range(fwd):
            late = LAG * (s + 1)
            if late < o_chunks:
                @pl.when(j >= late)
                def _(s=s, late=late):
                    h_hop(j - late, s)
        return carry

    lax.fori_loop(0, o_chunks, o_step, 0)

    def put(j, half):
        cols = half * o_chunks + j
        return pltpu.make_async_copy(h_all.at[:, cols], h_out.at[:, cols], out_sem.at[j, half])

    done = []
    for t in range(o_chunks, o_chunks + LAG * fwd):
        for s in reversed(range(fwd)):
            j = t - LAG * (s + 1)
            if 0 <= j < o_chunks:
                h_hop(j, s)
                if s + 1 == fwd:
                    done.append(j)
    for j in done:
        put(j, core).start()
    for j in done:
        h_pair_in(j).wait_recv()
        put(j, other).start()
    table_out[...] = jnp.sum(tabs[...], axis=0)

    x_pair.wait_send()
    t_pair.wait_send()
    for args in small:
        for back, hops in ((0, fwd), (1, bwd)):
            for s in range(hops):
                ring(*args, s, back).wait_send()
    for copy in o_copies:
        copy.wait_send()
    for j in range(o_chunks):
        for s in range(fwd):
            for back in range(2):
                h_ring(j, s, back).wait_send()
        h_pair(j).wait_send()
        put(j, core).wait()
        put(j, other).wait()


def attend(x_loc, w_q, w_k, w_v, w_o, ids, probs, group):
    tok_dev, width = x_loc.shape
    chips = group // 2
    tok_chip = 2 * tok_dev
    heads_core = w_q.shape[1] // HEAD_DIM // 2
    kv_width = w_k.shape[1] // 2
    q_core = heads_core * HEAD_DIM
    lanes = probs.shape[1]
    table_rows = 4 * chips * tok_chip // lanes
    o_chunks = width // 2 // COLS
    kv_core = kv_width // HEAD_DIM
    kv_units = 2 * kv_width // COLS * (width // ROWS)
    units = kv_units + (q_core // COLS) * (width // ROWS) + o_chunks * 2 * q_core // ROWS
    n_slots = units // 2
    bf16, f32 = jnp.bfloat16, jnp.float32
    dma = pltpu.SemaphoreType.DMA
    anywhere = pl.BlockSpec(memory_space=pl.ANY)
    in_vmem = pl.BlockSpec(memory_space=pltpu.VMEM)
    return pl.pallas_call(
        functools.partial(block_kernel, group),
        name='attend',
        in_specs=[anywhere] * 5 + [in_vmem] * 2,
        out_specs=[anywhere, in_vmem],
        out_shape=[jax.ShapeDtypeStruct((chips, width // COLS, tok_chip, COLS), bf16), jax.ShapeDtypeStruct((table_rows, lanes), f32)],
        scratch_shapes=[
            pltpu.VMEM((n_slots, ROWS, COLS), bf16),
            pltpu.VMEM((tok_chip, width), bf16),
            pltpu.VMEM((chips, 2, tok_chip, kv_width), bf16),
            pltpu.VMEM((heads_core, tok_chip, HEAD_DIM), bf16),
            pltpu.VMEM((2, tok_chip, q_core), bf16),
            pltpu.VMEM((chips, width // COLS, tok_chip, COLS), bf16),
            pltpu.VMEM((2, table_rows, lanes), f32),
            pltpu.VMEM((chips, table_rows, lanes), f32),
            dma((n_slots,)), dma, dma((2,)), dma((2,)), dma((8,)), dma((8,)), dma((8,)), dma((8,)), dma((kv_core,)), dma((kv_core,)),
            dma((o_chunks, 8)), dma((o_chunks, 8)), dma((o_chunks,)), dma((o_chunks,)), dma((o_chunks, 2)),
        ],
        compiler_params=pltpu.CompilerParams(collective_id=0, has_side_effects=True, vmem_limit_bytes=65_000_000),
    )(x_loc, w_q, w_k, w_v, w_o, ids, probs)


def solution(mesh):
    group = mesh.shape['sp']
    row_spec = P(('dp', 'sp'), None)
    buf_spec = P(('dp', 'sp'), None, None)

    def device_step(x_loc, w_q, w_k, w_v, w_o, ids_loc, probs_loc):
        h_all, table = attend(x_loc, w_q, w_k, w_v, w_o, ids_loc, probs_loc, group)
        buf, hid = build_buffers(h_all, table, x_loc.shape[0], probs_loc.shape[1] // group)
        return hid, buf

    return jax.shard_map(device_step, mesh=mesh, in_specs=(row_spec, P(), P(), P(), P(), row_spec, row_spec), out_specs=(row_spec, buf_spec), check_vma=False)
```

```python
import math
import functools
import jax
import jax.numpy as jnp
from jax import lax
from jax.experimental import pallas as pl
from jax.experimental.pallas import tpu as pltpu
from jax.sharding import PartitionSpec as P

HEAD_DIM = 128
SCORE_SCALE = 1.0 / math.sqrt(HEAD_DIM)
COLS = 256
ROWS = 2048
LAG = 2
CHAIN = 4
GROUP_ROWS = 128
MESH = pl.DeviceIdType.MESH


def route_table(me, ids, probs, seq, table_rows):
    tok_dev, lanes = probs.shape
    per_row = lanes // tok_dev
    sub = lax.broadcasted_iota(jnp.int32, (tok_dev, lanes), 0)
    lane = lax.broadcasted_iota(jnp.int32, (tok_dev, lanes), 1)
    tok = lane - tok_dev * lax.rem(me, per_row)
    diag = tok == sub
    square = lax.broadcasted_iota(jnp.int32, (tok_dev, tok_dev), 0) == lax.broadcasted_iota(jnp.int32, (tok_dev, tok_dev), 1)
    ids = ids.astype(jnp.float32)
    e_sub = [jnp.sum(jnp.where(square, ids[k:k + 1, :], 0.0), axis=1, keepdims=True) for k in range(2)]
    lane_f = lane.astype(jnp.float32)
    p_sub = [jnp.sum(jnp.where(lane_f == e, probs, 0.0), axis=1, keepdims=True) for e in e_sub]
    total = p_sub[0] + p_sub[1]
    to_lanes = lambda col: jnp.sum(jnp.where(diag, col, 0.0), axis=0, keepdims=True)
    e_lane = [to_lanes(e) for e in e_sub]
    valid = jnp.sum(jnp.where(diag, 1.0, 0.0), axis=0, keepdims=True)
    base = (tok_dev * me).astype(jnp.float32)
    dests, gates = [], []
    for k in range(2):
        same = ((e_sub[0] == e_lane[k]) | (e_sub[1] == e_lane[k])) & (sub < tok)
        slot = jnp.sum(jnp.where(same, 1.0, 0.0), axis=0, keepdims=True)
        dests.append(valid * (e_lane[k] * float(seq) + base + slot))
        gates.append(to_lanes(p_sub[k] / total))
    row = lax.broadcasted_iota(jnp.int32, (table_rows, lanes), 0)
    mine = lax.div(me, per_row)
    n_rows = table_rows // 4
    table = jnp.zeros((table_rows, lanes), jnp.float32)
    for n, vec in enumerate(dests + gates):
        table = jnp.where(row == n * n_rows + mine, vec, table)
    return table


def build_kernel(h_ref, table_ref, out_ref, hid_ref, zeros, slots, hid_buf, sems, hid_sem):
    me = lax.axis_index('sp')
    experts_dev, seq, width = out_ref.shape
    n_chips, n_cols, tok_chip, cols = h_ref.shape
    tok_dev = hid_ref.shape[0]
    n_groups = sems.shape[0]
    per_expert = n_groups // experts_dev
    n_rows = table_ref.shape[0] // 4
    lanes = table_ref.shape[1]

    per_chip = tok_chip // tok_dev
    chip = lax.div(me, per_chip)
    first = pl.multiple_of(lax.rem(me, per_chip) * tok_dev, tok_dev)
    for n in range(n_cols):
        hid_buf[:, n * cols:(n + 1) * cols] = h_ref[chip, n, pl.ds(first, tok_dev), :]
    hid_copy = pltpu.make_async_copy(hid_buf, hid_ref, hid_sem)
    hid_copy.start()
    zeros[...] = jnp.zeros_like(zeros)

    table = table_ref[...]
    base = me * experts_dev * seq
    group_first = (base + GROUP_ROWS * lax.broadcasted_iota(jnp.int32, (n_groups, lanes), 0)).astype(jnp.float32)
    hits = jnp.zeros((n_groups, lanes), jnp.float32)
    for r in range(2 * n_rows):
        dest = table[r:r + 1, :]
        hits = jnp.where((dest >= group_first) & (dest < group_first + float(GROUP_ROWS)), 1.0, hits)
    used = jnp.max(hits, axis=1, keepdims=True)
    power = lax.shift_left(jnp.ones((n_groups, 1), jnp.int32), lax.broadcasted_iota(jnp.int32, (n_groups, 1), 0))
    used_bits = jnp.sum(used * power.astype(jnp.float32)).astype(jnp.int32)

    def is_used(n):
        return lax.rem(lax.shift_right_logical(used_bits, n), 2) == 1

    def put(src, n):
        expert, part = lax.div(n, per_expert), lax.rem(n, per_expert)
        at = pl.ds(pl.multiple_of(part * GROUP_ROWS, GROUP_ROWS), GROUP_ROWS)
        return pltpu.make_async_copy(src, out_ref.at[expert, at], sems.at[n])

    def put_zeros(n, carry):
        @pl.when(jnp.logical_not(is_used(n)))
        def _():
            put(zeros, n).start()
        return carry

    lax.fori_loop(0, n_groups, put_zeros, 0)

    spread = lambda n: jnp.concatenate([table[n * n_rows + r:n * n_rows + r + 1, :] for r in range(n_rows)], axis=1)
    dest = [spread(0), spread(1)]
    gate = [spread(2), spread(3)]

    def put_rows(n, carry):
        @pl.when(is_used(n))
        def _():
            row = (lax.broadcasted_iota(jnp.int32, (GROUP_ROWS, seq), 0) + (base + n * GROUP_ROWS)).astype(jnp.float32)
            hit = [dest[0] == row, dest[1] == row]
            gate_row = jnp.sum(jnp.where(hit[0], gate[0], 0.0) + jnp.where(hit[1], gate[1], 0.0), axis=1, keepdims=True)
            pick = jnp.where(hit[0] | hit[1], 1.0, 0.0).astype(jnp.bfloat16)
            for c in range(n_cols):
                rows = h_ref[:, c].reshape(seq, cols)
                got = jnp.dot(pick, rows, preferred_element_type=jnp.float32)
                slots[n, :, c * cols:(c + 1) * cols] = (got * gate_row).astype(jnp.bfloat16)
            put(slots.at[n], n).start()
        return carry

    lax.fori_loop(0, n_groups, put_rows, 0)

    def wait_group(n, carry):
        put(zeros, n).wait()
        return carry

    lax.fori_loop(0, n_groups, wait_group, 0)
    hid_copy.wait()


def build_buffers(h_all, table, tok_dev, experts_dev):
    n_chips, n_cols, tok_chip, cols = h_all.shape
    seq, width = n_chips * tok_chip, n_cols * cols
    n_groups = experts_dev * seq // GROUP_ROWS
    bf16 = jnp.bfloat16
    in_vmem = pl.BlockSpec(memory_space=pltpu.VMEM)
    anywhere = pl.BlockSpec(memory_space=pl.ANY)
    dma = pltpu.SemaphoreType.DMA
    return pl.pallas_call(
        build_kernel,
        name='build_buffers',
        in_specs=[in_vmem, in_vmem],
        out_specs=[anywhere, anywhere],
        out_shape=[jax.ShapeDtypeStruct((experts_dev, seq, width), bf16), jax.ShapeDtypeStruct((tok_dev, width), bf16)],
        scratch_shapes=[
            pltpu.VMEM((GROUP_ROWS, width), bf16), pltpu.VMEM((n_groups, GROUP_ROWS, width), bf16), pltpu.VMEM((tok_dev, width), bf16),
            dma((n_groups,)), dma,
        ],
        compiler_params=pltpu.CompilerParams(vmem_limit_bytes=40 * 1024 * 1024),
        cost_estimate=pl.CostEstimate(flops=2 * experts_dev * seq * seq * width, bytes_accessed=2 * experts_dev * seq * width, transcendentals=0),
    )(h_all, table)


def block_kernel(x_hbm, wq, wk, wv, wo, ids_hbm, probs_hbm, h_all, table_out, wbuf, x_buf, kv, q_buf, o_buf, tab_pair, tabs, ids, probs,
                 w_sem, in_sem, pair_send, pair_recv, kv_send, kv_recv, tab_send, tab_recv, o_send, o_recv, h_send, h_recv, d_send, d_recv):
    tok_dev, width = x_hbm.shape
    chips = kv.shape[0]
    tok_chip = x_buf.shape[0]
    seq = chips * tok_chip
    heads_core = q_buf.shape[0]
    kv_core = kv.shape[3] // HEAD_DIM
    per_kv = heads_core // kv_core
    q_core = heads_core * HEAD_DIM
    out_core = width // 2
    fwd, bwd = chips // 2, chips // 2 - 1
    me = lax.axis_index('sp')
    chip, core = lax.div(me, 2), lax.rem(me, 2)
    other = 1 - core
    partner = {'sp': 2 * chip + other}

    def far(step):
        return {'sp': 2 * lax.rem(chip + chips + step, chips) + core}

    def remote(src, dst, send, recv, device):
        return pltpu.make_async_remote_copy(src_ref=src, dst_ref=dst, send_sem=send, recv_sem=recv, device_id=device, device_id_type=MESH)

    barrier = pltpu.get_barrier_semaphore()
    near = [partner, far(1), far(-1), far(2), far(-2)]
    for device in near:
        pl.semaphore_signal(barrier, inc=1, device_id=device, device_id_type=MESH)

    n_slots = wbuf.shape[0]
    kv_units = 2 * (kv.shape[3] // COLS) * (width // ROWS)
    half_units = q_core // ROWS
    chunk_units = 2 * half_units
    in_units = width // ROWS
    q_chunks = q_core // COLS
    o_chunks = out_core // COLS
    kv_chunks = kv.shape[3] // COLS

    def load(src, row, col, slot):
        return pltpu.make_async_copy(src.at[pl.ds(row, ROWS), pl.ds(pl.multiple_of(col, COLS), COLS)], wbuf.at[slot], w_sem.at[slot])

    def wait_unit(slot):
        load(wk, 0, 0, slot).wait()

    def start_q(n):
        for r in range(in_units):
            load(wq, r * ROWS, core * q_core + n * COLS, lax.rem(kv_units + in_units * n + r, n_slots)).start()

    first_o = kv_units + in_units * q_chunks - n_slots

    def start_o(k):
        j, r = lax.div(k, chunk_units), lax.rem(k, chunk_units)
        half = jnp.where(r < half_units, core, other)
        row = pl.multiple_of(half * q_core + lax.rem(r, half_units) * ROWS, ROWS)
        load(wo, row, core * out_core + j * COLS, first_o + k).start()

    own = pl.ds(pl.multiple_of(core * tok_dev, tok_dev), tok_dev)
    theirs = pl.ds(pl.multiple_of(other * tok_dev, tok_dev), tok_dev)
    x_in = pltpu.make_async_copy(x_hbm, x_buf.at[own], in_sem.at[0])
    x_in.start()
    slot = 0
    for src in (wk, wv):
        for n in range(kv_chunks):
            for r in range(in_units):
                load(src, r * ROWS, core * kv.shape[3] + n * COLS, slot).start()
                slot += 1
    ids_in = pltpu.make_async_copy(ids_hbm, ids, in_sem.at[1])
    probs_in = pltpu.make_async_copy(probs_hbm, probs, in_sem.at[2])
    ids_in.start()
    probs_in.start()
    x_in.wait()
    pl.semaphore_wait(barrier, len(near))

    x_pair = remote(x_buf.at[own], x_buf.at[own], pair_send.at[0], pair_recv.at[0], partner)
    x_pair.start()
    q_first = (n_slots - kv_units) // in_units
    lax.fori_loop(0, q_first, lambda n, c: (start_q(n), c)[1], 0)
    remote(x_buf.at[theirs], x_buf.at[theirs], pair_send.at[0], pair_recv.at[0], partner).wait_recv()

    def project(pair_slot):
        for r in range(in_units):
            wait_unit(pair_slot + r)
        w = wbuf[pl.ds(pair_slot, in_units)].reshape(width, COLS)
        return jnp.dot(x_buf[...], w, preferred_element_type=jnp.float32).astype(jnp.bfloat16)

    def kv_piece(block, which):
        return kv.at[block, which]

    def tab_piece(block, which):
        return tabs.at[block]

    def ring(piece, sends, recvs, which, s, back, arriving=0):
        s_at = s + arriving
        block = lax.rem(chip + s_at, chips) if back else lax.rem(chip + chips - s_at, chips)
        part = piece(block, which)
        return remote(part, part, sends.at[which, 4 * back + s], recvs.at[which, 4 * back + s], far(-1) if back else far(1))

    def ring_start(*args):
        ring(*args, 0, 0).start()
        ring(*args, 0, 1).start()

    def ring_hop(*args):
        *args, s = args
        ring(*args, s, 0, 1).wait_recv()
        if s + 1 < fwd:
            ring(*args, s + 1, 0).start()
        if s < bwd:
            ring(*args, s, 1, 1).wait_recv()
            if s + 1 < bwd:
                ring(*args, s + 1, 1).start()

    kv_ring = (kv_piece, kv_send, kv_recv)
    tab_ring = (tab_piece, tab_send, tab_recv)

    slot = 0
    for which in range(2):
        for n in range(kv_chunks):
            kv[chip, which, :, n * COLS:(n + 1) * COLS] = project(slot)
            slot += in_units
        ring_start(*kv_ring, which)

    for n in range(q_first, q_chunks):
        start_q(n)
    early = kv_units - first_o
    for k in range(early):
        start_o(k)

    ids_in.wait()
    probs_in.wait()
    tab_pair[0] = route_table(me, ids[...], probs[...], seq, tab_pair.shape[1])
    t_pair = remote(tab_pair.at[0], tab_pair.at[1], pair_send.at[1], pair_recv.at[1], partner)
    t_pair.start()

    heads_chunk = COLS // HEAD_DIM

    def q_step(n, carry):
        res = project(lax.rem(kv_units + in_units * n, n_slots))
        for i in range(heads_chunk):
            q_buf[heads_chunk * n + i] = res[:, i * HEAD_DIM:(i + 1) * HEAD_DIM]

        @pl.when(n < q_first)
        def _():
            for r in range(in_units):
                start_o(early + in_units * n + r)
        return carry

    at = 0
    for s in range(fwd):
        for which in range(2):
            upto = q_chunks * (2 * s + which + 1) // (2 * fwd)
            upto = min(q_chunks, upto + (1 if s == 0 else 0))
            lax.fori_loop(at, upto, q_step, 0)
            at = upto
            ring_hop(*kv_ring, which, s)
        if s == 0:
            t_pair.wait_recv()
            tabs[chip] = tab_pair[0] + tab_pair[1]
            ring_start(*tab_ring, 0)
        else:
            ring_hop(*tab_ring, 0, s - 1)

    rows = per_kv * tok_chip
    q_pos = tok_chip * chip + lax.rem(lax.broadcasted_iota(jnp.int32, (rows, seq), 0), tok_chip)
    seen = lax.broadcasted_iota(jnp.int32, (rows, seq), 1) <= q_pos
    o_copies = []
    for g in range(kv_core):
        lanes = slice(g * HEAD_DIM, (g + 1) * HEAD_DIM)
        qg = q_buf[g * per_kv:(g + 1) * per_kv].reshape(rows, HEAD_DIM)
        kg = kv[:, 0, :, lanes].reshape(seq, HEAD_DIM)
        vg = kv[:, 1, :, lanes].reshape(seq, HEAD_DIM)
        s = lax.dot_general(qg, kg, (((1,), (1,)), ((), ())), preferred_element_type=jnp.float32) * SCORE_SCALE
        s = jnp.where(seen, s, -1e30)
        p = jnp.exp(s - jnp.max(s, axis=1, keepdims=True))
        p = (p / jnp.sum(p, axis=1, keepdims=True)).astype(jnp.bfloat16)
        o = jnp.dot(p, vg, preferred_element_type=jnp.float32).astype(jnp.bfloat16)
        for h in range(per_kv):
            col = (g * per_kv + h) * HEAD_DIM
            o_buf[0, :, col:col + HEAD_DIM] = o[h * tok_chip:(h + 1) * tok_chip]
        span = pl.ds(g * per_kv * HEAD_DIM, per_kv * HEAD_DIM)
        copy = remote(o_buf.at[0, :, span], o_buf.at[1, :, span], o_send.at[g], o_recv.at[g], partner)
        copy.start()
        o_copies.append(copy)
    ring_hop(*tab_ring, 0, fwd - 1)

    def h_copy(j, source, reach, step, back):
        block = lax.rem(chip + source, chips) if back else lax.rem(chip + chips - source, chips)
        piece = h_all.at[block, core * o_chunks + j]
        if reach == fwd:
            piece = piece.at[pl.ds(back * tok_dev, tok_dev)]
        n = 4 * back + reach - 1
        return remote(piece, piece, h_send.at[j, n], h_recv.at[j, n], far(-step) if back else far(step))

    def h_sends(j):
        if j < CHAIN:
            return [(reach - 1, reach, 1) for reach in range(1, fwd + 1)]
        return [(0, 1, 1), (0, 2, 2)] + [(2, reach, reach - 2) for reach in range(3, fwd + 1)]

    def h_start(j, source):
        for back in range(2):
            for src, reach, step in h_sends(j):
                if src == source:
                    h_copy(j, src, reach, step, back).start()

    def h_arrive(j, reach):
        for back in range(2):
            h_copy(j, reach, reach, 1, back).wait_recv()
            for src, onward, step in h_sends(j):
                if src == reach:
                    h_copy(j, src, onward, step, back).start()
        if reach == fwd:
            h_pair(j, core).start()

    def h_pair(j, half):
        cols = h_all.at[:, half * o_chunks + j]
        return remote(cols, cols, d_send.at[j], d_recv.at[j], partner)

    def due(t):
        steps = []
        for j in range(o_chunks):
            for reach in range(1, fwd + 1):
                when = j + LAG * reach if j < CHAIN else j + LAG * (2 if reach > 2 else 1)
                if when == t:
                    steps.append((j, reach))
        return steps

    for j in range(o_chunks):
        at = first_o + chunk_units * j
        for r in range(half_units):
            wait_unit(at + r)
        acc = jnp.dot(o_buf[0], wbuf[pl.ds(at, half_units)].reshape(q_core, COLS), preferred_element_type=jnp.float32)
        if j == 0:
            for copy in o_copies:
                copy.wait_recv()
        for r in range(half_units):
            wait_unit(at + half_units + r)
        acc += jnp.dot(o_buf[1], wbuf[pl.ds(at + half_units, half_units)].reshape(q_core, COLS), preferred_element_type=jnp.float32)
        x_cols = x_buf[:, pl.ds(pl.multiple_of(core * out_core + j * COLS, COLS), COLS)]
        h_all[chip, core * o_chunks + j] = (x_cols.astype(jnp.float32) + acc).astype(jnp.bfloat16)
        h_start(j, 0)
        for step in due(j):
            h_arrive(*step)

    table_out[...] = jnp.sum(tabs[...], axis=0)
    for t in range(o_chunks, o_chunks + LAG * fwd):
        for step in due(t):
            h_arrive(*step)
    for j in range(o_chunks):
        h_pair(j, other).wait_recv()

    x_pair.wait_send()
    t_pair.wait_send()
    for args in ((*kv_ring, 0), (*kv_ring, 1), (*tab_ring, 0)):
        for back, hops in ((0, fwd), (1, bwd)):
            for s in range(hops):
                ring(*args, s, back).wait_send()
    for copy in o_copies:
        copy.wait_send()
    for j in range(o_chunks):
        for back in range(2):
            for src, reach, step in h_sends(j):
                h_copy(j, src, reach, step, back).wait_send()
        h_pair(j, core).wait_send()


def attend(x_loc, w_q, w_k, w_v, w_o, ids, probs, group):
    tok_dev, width = x_loc.shape
    chips = group // 2
    tok_chip = 2 * tok_dev
    heads_core = w_q.shape[1] // HEAD_DIM // 2
    kv_width = w_k.shape[1] // 2
    q_core = heads_core * HEAD_DIM
    lanes = probs.shape[1]
    table_rows = 4 * chips * tok_chip // lanes
    o_chunks = width // 2 // COLS
    kv_core = kv_width // HEAD_DIM
    kv_units = 2 * kv_width // COLS * (width // ROWS)
    units = kv_units + (q_core // COLS) * (width // ROWS) + o_chunks * 2 * q_core // ROWS
    n_slots = units // 2
    bf16, f32 = jnp.bfloat16, jnp.float32
    dma = pltpu.SemaphoreType.DMA
    anywhere = pl.BlockSpec(memory_space=pl.ANY)
    in_vmem = pl.BlockSpec(memory_space=pltpu.VMEM)
    return pl.pallas_call(
        block_kernel,
        name='attend',
        in_specs=[anywhere] * 7,
        out_specs=[in_vmem, in_vmem],
        out_shape=[pltpu.VMEM((chips, width // COLS, tok_chip, COLS), bf16), pltpu.VMEM((table_rows, lanes), f32)],
        scratch_shapes=[
            pltpu.VMEM((n_slots, ROWS, COLS), bf16),
            pltpu.VMEM((tok_chip, width), bf16),
            pltpu.VMEM((chips, 2, tok_chip, kv_width), bf16),
            pltpu.VMEM((heads_core, tok_chip, HEAD_DIM), bf16),
            pltpu.VMEM((2, tok_chip, q_core), bf16),
            pltpu.VMEM((2, table_rows, lanes), f32),
            pltpu.VMEM((chips, table_rows, lanes), f32),
            pltpu.VMEM(ids.shape, ids.dtype),
            pltpu.VMEM(probs.shape, probs.dtype),
            dma((n_slots,)), dma((3,)), dma((2,)), dma((2,)), dma((2, 8)), dma((2, 8)), dma((1, 8)), dma((1, 8)), dma((kv_core,)), dma((kv_core,)),
            dma((o_chunks, 8)), dma((o_chunks, 8)), dma((o_chunks,)), dma((o_chunks,)),
        ],
        compiler_params=pltpu.CompilerParams(collective_id=0, has_side_effects=True, vmem_limit_bytes=60_000_000),
    )(x_loc, w_q, w_k, w_v, w_o, ids, probs)


def solution(mesh):
    group = mesh.shape['sp']
    row_spec = P(('dp', 'sp'), None)
    buf_spec = P(('dp', 'sp'), None, None)

    def device_step(x_loc, w_q, w_k, w_v, w_o, ids_loc, probs_loc):
        h_all, table = attend(x_loc, w_q, w_k, w_v, w_o, ids_loc.T, probs_loc, group)
        buf, hid = build_buffers(h_all, table, x_loc.shape[0], probs_loc.shape[1] // group)
        return hid, buf

    return jax.shard_map(device_step, mesh=mesh, in_specs=(row_spec, P(), P(), P(), P(), row_spec, row_spec), out_specs=(row_spec, buf_spec), check_vma=False)
```

```python
import math
import functools
import jax
import jax.numpy as jnp
from jax import lax
from jax.experimental import pallas as pl
from jax.experimental.pallas import tpu as pltpu
from jax.sharding import PartitionSpec as P

HEAD_DIM = 128
SCORE_SCALE = 1.0 / math.sqrt(HEAD_DIM)
COLS = 256
ROWS = 2048
LAG = 2
Q_STOPS = (8, 11)
CHAIN = 3
GROUP_ROWS = 128
MESH = pl.DeviceIdType.MESH


def route_table(me, ids, probs, seq, table_rows):
    tok_dev, lanes = probs.shape
    per_row = lanes // tok_dev
    sub = lax.broadcasted_iota(jnp.int32, (tok_dev, lanes), 0)
    lane = lax.broadcasted_iota(jnp.int32, (tok_dev, lanes), 1)
    tok = lane - tok_dev * lax.rem(me, per_row)
    diag = tok == sub
    square = lax.broadcasted_iota(jnp.int32, (tok_dev, tok_dev), 0) == lax.broadcasted_iota(jnp.int32, (tok_dev, tok_dev), 1)
    ids = ids.astype(jnp.float32)
    e_sub = [jnp.sum(jnp.where(square, ids[k:k + 1, :], 0.0), axis=1, keepdims=True) for k in range(2)]
    lane_f = lane.astype(jnp.float32)
    p_sub = [jnp.sum(jnp.where(lane_f == e, probs, 0.0), axis=1, keepdims=True) for e in e_sub]
    total = p_sub[0] + p_sub[1]
    to_lanes = lambda col: jnp.sum(jnp.where(diag, col, 0.0), axis=0, keepdims=True)
    e_lane = [to_lanes(e) for e in e_sub]
    valid = jnp.sum(jnp.where(diag, 1.0, 0.0), axis=0, keepdims=True)
    base = (tok_dev * me).astype(jnp.float32)
    dests, gates = [], []
    for k in range(2):
        same = ((e_sub[0] == e_lane[k]) | (e_sub[1] == e_lane[k])) & (sub < tok)
        slot = jnp.sum(jnp.where(same, 1.0, 0.0), axis=0, keepdims=True)
        dests.append(valid * (e_lane[k] * float(seq) + base + slot))
        gates.append(to_lanes(p_sub[k] / total))
    row = lax.broadcasted_iota(jnp.int32, (table_rows, lanes), 0)
    mine = lax.div(me, per_row)
    n_rows = table_rows // 4
    table = jnp.zeros((table_rows, lanes), jnp.float32)
    for n, vec in enumerate(dests + gates):
        table = jnp.where(row == n * n_rows + mine, vec, table)
    return table


def build_kernel(h_ref, table_ref, out_ref, hid_ref, zeros, slots, hid_buf, sems, hid_sem):
    me = lax.axis_index('sp')
    experts_dev, seq, width = out_ref.shape
    n_chips, n_cols, tok_chip, cols = h_ref.shape
    tok_dev = hid_ref.shape[0]
    n_groups = sems.shape[0]
    per_expert = n_groups // experts_dev
    n_rows = table_ref.shape[0] // 4
    lanes = table_ref.shape[1]

    per_chip = tok_chip // tok_dev
    chip = lax.div(me, per_chip)
    first = pl.multiple_of(lax.rem(me, per_chip) * tok_dev, tok_dev)
    for n in range(n_cols):
        hid_buf[:, n * cols:(n + 1) * cols] = h_ref[chip, n, pl.ds(first, tok_dev), :]
    hid_copy = pltpu.make_async_copy(hid_buf, hid_ref, hid_sem)
    hid_copy.start()
    zeros[...] = jnp.zeros_like(zeros)

    table = table_ref[...]
    base = me * experts_dev * seq
    group_first = (base + GROUP_ROWS * lax.broadcasted_iota(jnp.int32, (n_groups, lanes), 0)).astype(jnp.float32)
    hits = jnp.zeros((n_groups, lanes), jnp.float32)
    for r in range(2 * n_rows):
        dest = table[r:r + 1, :]
        hits = jnp.where((dest >= group_first) & (dest < group_first + float(GROUP_ROWS)), 1.0, hits)
    used = jnp.max(hits, axis=1, keepdims=True)
    power = lax.shift_left(jnp.ones((n_groups, 1), jnp.int32), lax.broadcasted_iota(jnp.int32, (n_groups, 1), 0))
    used_bits = jnp.sum(used * power.astype(jnp.float32)).astype(jnp.int32)

    def is_used(n):
        return lax.rem(lax.shift_right_logical(used_bits, n), 2) == 1

    def put(src, n):
        expert, part = lax.div(n, per_expert), lax.rem(n, per_expert)
        at = pl.ds(pl.multiple_of(part * GROUP_ROWS, GROUP_ROWS), GROUP_ROWS)
        return pltpu.make_async_copy(src, out_ref.at[expert, at], sems.at[n])

    def put_zeros(n, carry):
        @pl.when(jnp.logical_not(is_used(n)))
        def _():
            put(zeros, n).start()
        return carry

    lax.fori_loop(0, n_groups, put_zeros, 0)

    spread = lambda n: jnp.concatenate([table[n * n_rows + r:n * n_rows + r + 1, :] for r in range(n_rows)], axis=1)
    dest = [spread(0), spread(1)]
    gate = [spread(2), spread(3)]

    def put_rows(n, carry):
        @pl.when(is_used(n))
        def _():
            row = (lax.broadcasted_iota(jnp.int32, (GROUP_ROWS, seq), 0) + (base + n * GROUP_ROWS)).astype(jnp.float32)
            hit = [dest[0] == row, dest[1] == row]
            gate_row = jnp.sum(jnp.where(hit[0], gate[0], 0.0) + jnp.where(hit[1], gate[1], 0.0), axis=1, keepdims=True)
            pick = jnp.where(hit[0] | hit[1], 1.0, 0.0).astype(jnp.bfloat16)
            for c in range(n_cols):
                rows = h_ref[:, c].reshape(seq, cols)
                got = jnp.dot(pick, rows, preferred_element_type=jnp.float32)
                slots[n, :, c * cols:(c + 1) * cols] = (got * gate_row).astype(jnp.bfloat16)
            put(slots.at[n], n).start()
        return carry

    lax.fori_loop(0, n_groups, put_rows, 0)

    def wait_group(n, carry):
        put(zeros, n).wait()
        return carry

    lax.fori_loop(0, n_groups, wait_group, 0)
    hid_copy.wait()


def build_buffers(h_all, table, tok_dev, experts_dev):
    n_chips, n_cols, tok_chip, cols = h_all.shape
    seq, width = n_chips * tok_chip, n_cols * cols
    n_groups = experts_dev * seq // GROUP_ROWS
    bf16 = jnp.bfloat16
    in_vmem = pl.BlockSpec(memory_space=pltpu.VMEM)
    anywhere = pl.BlockSpec(memory_space=pl.ANY)
    dma = pltpu.SemaphoreType.DMA
    return pl.pallas_call(
        build_kernel,
        name='build_buffers',
        in_specs=[in_vmem, in_vmem],
        out_specs=[anywhere, anywhere],
        out_shape=[jax.ShapeDtypeStruct((experts_dev, seq, width), bf16), jax.ShapeDtypeStruct((tok_dev, width), bf16)],
        scratch_shapes=[
            pltpu.VMEM((GROUP_ROWS, width), bf16), pltpu.VMEM((n_groups, GROUP_ROWS, width), bf16), pltpu.VMEM((tok_dev, width), bf16),
            dma((n_groups,)), dma,
        ],
        compiler_params=pltpu.CompilerParams(vmem_limit_bytes=40 * 1024 * 1024),
        cost_estimate=pl.CostEstimate(flops=2 * experts_dev * seq * seq * width, bytes_accessed=2 * experts_dev * seq * width, transcendentals=0),
    )(h_all, table)


def block_kernel(x_hbm, wq, wk, wv, wo, ids_hbm, probs_hbm, h_all, table_out, wbuf, x_buf, kv, q_buf, o_buf, tab_pair, tabs, ids, probs,
                 w_sem, in_sem, pair_send, pair_recv, kv_send, kv_recv, tab_send, tab_recv, o_send, o_recv, h_send, h_recv, d_send, d_recv):
    tok_dev, width = x_hbm.shape
    chips = kv.shape[0]
    tok_chip = x_buf.shape[0]
    seq = chips * tok_chip
    heads_core = q_buf.shape[0]
    kv_core = kv.shape[3] // HEAD_DIM
    per_kv = heads_core // kv_core
    q_core = heads_core * HEAD_DIM
    out_core = width // 2
    fwd, bwd = chips // 2, chips // 2 - 1
    me = lax.axis_index('sp')
    chip, core = lax.div(me, 2), lax.rem(me, 2)
    other = 1 - core
    partner = {'sp': 2 * chip + other}

    def far(step):
        return {'sp': 2 * lax.rem(chip + chips + step, chips) + core}

    def remote(src, dst, send, recv, device):
        return pltpu.make_async_remote_copy(src_ref=src, dst_ref=dst, send_sem=send, recv_sem=recv, device_id=device, device_id_type=MESH)

    barrier = pltpu.get_barrier_semaphore()
    near = [partner, far(1), far(-1), far(2), far(-2)]
    for device in near:
        pl.semaphore_signal(barrier, inc=1, device_id=device, device_id_type=MESH)

    n_slots = wbuf.shape[0]
    kv_units = 2 * (kv.shape[3] // COLS) * (width // ROWS)
    half_units = q_core // ROWS
    chunk_units = 2 * half_units
    in_units = width // ROWS
    q_chunks = q_core // COLS
    o_chunks = out_core // COLS
    kv_chunks = kv.shape[3] // COLS

    def load(src, row, col, slot):
        return pltpu.make_async_copy(src.at[pl.ds(row, ROWS), pl.ds(pl.multiple_of(col, COLS), COLS)], wbuf.at[slot], w_sem.at[slot])

    def wait_unit(slot):
        load(wk, 0, 0, slot).wait()

    def start_q(n):
        for r in range(in_units):
            load(wq, r * ROWS, core * q_core + n * COLS, lax.rem(kv_units + in_units * n + r, n_slots)).start()

    first_o = kv_units + in_units * q_chunks - n_slots

    def start_o(k):
        j, r = lax.div(k, chunk_units), lax.rem(k, chunk_units)
        half = jnp.where(r < half_units, core, other)
        row = pl.multiple_of(half * q_core + lax.rem(r, half_units) * ROWS, ROWS)
        load(wo, row, core * out_core + j * COLS, first_o + k).start()

    own = pl.ds(pl.multiple_of(core * tok_dev, tok_dev), tok_dev)
    theirs = pl.ds(pl.multiple_of(other * tok_dev, tok_dev), tok_dev)
    x_in = pltpu.make_async_copy(x_hbm, x_buf.at[own], in_sem.at[0])
    x_in.start()
    slot = 0
    for src in (wk, wv):
        for n in range(kv_chunks):
            for r in range(in_units):
                load(src, r * ROWS, core * kv.shape[3] + n * COLS, slot).start()
                slot += 1
    ids_in = pltpu.make_async_copy(ids_hbm, ids, in_sem.at[1])
    probs_in = pltpu.make_async_copy(probs_hbm, probs, in_sem.at[2])
    ids_in.start()
    probs_in.start()
    x_in.wait()
    pl.semaphore_wait(barrier, len(near))

    x_pair = remote(x_buf.at[own], x_buf.at[own], pair_send.at[0], pair_recv.at[0], partner)
    x_pair.start()
    q_first = (n_slots - kv_units) // in_units
    lax.fori_loop(0, q_first, lambda n, c: (start_q(n), c)[1], 0)
    remote(x_buf.at[theirs], x_buf.at[theirs], pair_send.at[0], pair_recv.at[0], partner).wait_recv()

    def project(pair_slot):
        for r in range(in_units):
            wait_unit(pair_slot + r)
        w = wbuf[pl.ds(pair_slot, in_units)].reshape(width, COLS)
        return jnp.dot(x_buf[...], w, preferred_element_type=jnp.float32).astype(jnp.bfloat16)

    def two_step(piece, sends, recvs, n, source, reach, step, back):
        block = lax.rem(chip + source, chips) if back else lax.rem(chip + chips - source, chips)
        part = piece(block, n)
        if reach == fwd:
            part = part.at[pl.ds(back * tok_dev, tok_dev)]
        at = 4 * back + reach - 1
        return remote(part, part, sends.at[n, at], recvs.at[n, at], far(-step) if back else far(step))

    def two_step_start(*args):
        for reach in (1, 2):
            for back in range(2):
                two_step(*args, 0, reach, reach, back).start()

    def two_step_onward(*args):
        for back in range(2):
            two_step(*args, 2, 2, 2, back).wait_recv()
            for reach in range(3, fwd + 1):
                two_step(*args, 2, reach, reach - 2, back).start()
        for back in range(2):
            two_step(*args, 1, 1, 1, back).wait_recv()

    def two_step_last(*args):
        for reach in range(3, fwd + 1):
            for back in range(2):
                two_step(*args, reach, reach, 1, back).wait_recv()

    def two_step_sent(*args):
        for back in range(2):
            for reach in range(1, fwd + 1):
                two_step(*args, 0 if reach < 3 else 2, reach, 1, back).wait_send()

    def kv_piece(block, which):
        return kv.at[block, which]

    def h_piece(block, j):
        return h_all.at[block, core * o_chunks + j]

    def tab_piece(block, which):
        return tabs.at[block]

    def ring(piece, sends, recvs, which, s, back, arriving=0):
        s_at = s + arriving
        block = lax.rem(chip + s_at, chips) if back else lax.rem(chip + chips - s_at, chips)
        part = piece(block, which)
        return remote(part, part, sends.at[which, 4 * back + s], recvs.at[which, 4 * back + s], far(-1) if back else far(1))

    def ring_start(*args):
        ring(*args, 0, 0).start()
        ring(*args, 0, 1).start()

    def ring_hop(*args):
        *args, s = args
        ring(*args, s, 0, 1).wait_recv()
        if s + 1 < fwd:
            ring(*args, s + 1, 0).start()
        if s < bwd:
            ring(*args, s, 1, 1).wait_recv()
            if s + 1 < bwd:
                ring(*args, s + 1, 1).start()

    kv_ring = (kv_piece, kv_send, kv_recv)
    tab_ring = (tab_piece, tab_send, tab_recv)

    slot = 0
    for which in range(2):
        for n in range(kv_chunks):
            kv[chip, which, :, n * COLS:(n + 1) * COLS] = project(slot)
            slot += in_units
        two_step_start(*kv_ring, which)

    for n in range(q_first, q_chunks):
        start_q(n)
    early = kv_units - first_o
    for k in range(early):
        start_o(k)

    ids_in.wait()
    probs_in.wait()
    tab_pair[0] = route_table(me, ids[...], probs[...], seq, tab_pair.shape[1])
    t_pair = remote(tab_pair.at[0], tab_pair.at[1], pair_send.at[1], pair_recv.at[1], partner)
    t_pair.start()

    heads_chunk = COLS // HEAD_DIM

    def q_step(n, carry):
        res = project(lax.rem(kv_units + in_units * n, n_slots))
        for i in range(heads_chunk):
            q_buf[heads_chunk * n + i] = res[:, i * HEAD_DIM:(i + 1) * HEAD_DIM]

        @pl.when(n < q_first)
        def _():
            for r in range(in_units):
                start_o(early + in_units * n + r)
        return carry

    lax.fori_loop(0, Q_STOPS[0], q_step, 0)
    t_pair.wait_recv()
    tabs[chip] = tab_pair[0] + tab_pair[1]
    ring_start(*tab_ring, 0)
    two_step_onward(*kv_ring, 0)
    lax.fori_loop(Q_STOPS[0], Q_STOPS[1], q_step, 0)
    two_step_onward(*kv_ring, 1)
    ring_hop(*tab_ring, 0, 0)
    lax.fori_loop(Q_STOPS[1], q_chunks, q_step, 0)
    ring_hop(*tab_ring, 0, 1)
    for which in range(2):
        two_step_last(*kv_ring, which)

    rows = per_kv * tok_chip
    q_pos = tok_chip * chip + lax.rem(lax.broadcasted_iota(jnp.int32, (rows, seq), 0), tok_chip)
    seen = lax.broadcasted_iota(jnp.int32, (rows, seq), 1) <= q_pos
    o_copies = []
    for g in range(kv_core):
        lanes = slice(g * HEAD_DIM, (g + 1) * HEAD_DIM)
        qg = q_buf[g * per_kv:(g + 1) * per_kv].reshape(rows, HEAD_DIM)
        kg = kv[:, 0, :, lanes].reshape(seq, HEAD_DIM)
        vg = kv[:, 1, :, lanes].reshape(seq, HEAD_DIM)
        s = lax.dot_general(qg, kg, (((1,), (1,)), ((), ())), preferred_element_type=jnp.float32) * SCORE_SCALE
        s = jnp.where(seen, s, -1e30)
        p = jnp.exp(s - jnp.max(s, axis=1, keepdims=True))
        p = (p / jnp.sum(p, axis=1, keepdims=True)).astype(jnp.bfloat16)
        o = jnp.dot(p, vg, preferred_element_type=jnp.float32).astype(jnp.bfloat16)
        for h in range(per_kv):
            col = (g * per_kv + h) * HEAD_DIM
            o_buf[0, :, col:col + HEAD_DIM] = o[h * tok_chip:(h + 1) * tok_chip]
        span = pl.ds(g * per_kv * HEAD_DIM, per_kv * HEAD_DIM)
        copy = remote(o_buf.at[0, :, span], o_buf.at[1, :, span], o_send.at[g], o_recv.at[g], partner)
        copy.start()
        o_copies.append(copy)
    ring_hop(*tab_ring, 0, 2)

    h_ring = (h_piece, h_send, h_recv)

    def chain_hop(j, reach):
        for back in range(2):
            two_step(*h_ring, j, reach, reach, 1, back).wait_recv()
            if reach < fwd:
                two_step(*h_ring, j, reach, reach + 1, 1, back).start()
        if reach == fwd:
            h_pair(j, core).start()

    def last_step(j):
        two_step_last(*h_ring, j)
        h_pair(j, core).start()

    def h_pair(j, half):
        cols = h_all.at[:, half * o_chunks + j]
        return remote(cols, cols, d_send.at[j], d_recv.at[j], partner)

    def o_step(j, carry):
        at = first_o + chunk_units * j
        for r in range(half_units):
            wait_unit(at + r)
        acc = jnp.dot(o_buf[0], wbuf[pl.ds(at, half_units)].reshape(q_core, COLS), preferred_element_type=jnp.float32)

        @pl.when(j == 0)
        def _():
            for copy in o_copies:
                copy.wait_recv()
        for r in range(half_units):
            wait_unit(at + half_units + r)
        acc += jnp.dot(o_buf[1], wbuf[pl.ds(at + half_units, half_units)].reshape(q_core, COLS), preferred_element_type=jnp.float32)
        x_cols = x_buf[:, pl.ds(pl.multiple_of(core * out_core + j * COLS, COLS), COLS)]
        h_all[chip, core * o_chunks + j] = (x_cols.astype(jnp.float32) + acc).astype(jnp.bfloat16)
        for back in range(2):
            two_step(*h_ring, j, 0, 1, 1, back).start()

        @pl.when(j >= CHAIN)
        def _():
            for back in range(2):
                two_step(*h_ring, j, 0, 2, 2, back).start()

        for reach in range(1, fwd):
            late = j - LAG * reach

            @pl.when((late >= 0) & (late < CHAIN))
            def _(late=late, reach=reach):
                chain_hop(late, reach)

        @pl.when(j >= CHAIN + LAG)
        def _():
            two_step_onward(*h_ring, j - LAG)

        @pl.when(j >= CHAIN + 2 * LAG)
        def _():
            last_step(j - 2 * LAG)
        return carry

    lax.fori_loop(0, o_chunks, o_step, 0)
    for reach in range(1, fwd):
        for j in range(max(0, o_chunks - LAG * reach), CHAIN):
            chain_hop(j, reach)
    for j in range(o_chunks - LAG, o_chunks):
        two_step_onward(*h_ring, j)
    ring_hop(*tab_ring, 0, fwd - 1)
    table_out[...] = jnp.sum(tabs[...], axis=0)
    for j in range(CHAIN):
        chain_hop(j, fwd)
    for j in range(max(CHAIN, o_chunks - 2 * LAG), o_chunks):
        last_step(j)
    for j in range(o_chunks):
        h_pair(j, other).wait_recv()

    x_pair.wait_send()
    t_pair.wait_send()
    for back, hops in ((0, fwd), (1, bwd)):
        for n in range(hops):
            ring(*tab_ring, 0, n, back).wait_send()
    for which in range(2):
        two_step_sent(*kv_ring, which)
    for copy in o_copies:
        copy.wait_send()

    def sent(j, carry):
        two_step_sent(*h_ring, j)
        h_pair(j, core).wait_send()
        return carry

    lax.fori_loop(0, o_chunks, sent, 0)


def attend(x_loc, w_q, w_k, w_v, w_o, ids, probs, group):
    tok_dev, width = x_loc.shape
    chips = group // 2
    tok_chip = 2 * tok_dev
    heads_core = w_q.shape[1] // HEAD_DIM // 2
    kv_width = w_k.shape[1] // 2
    q_core = heads_core * HEAD_DIM
    lanes = probs.shape[1]
    table_rows = 4 * chips * tok_chip // lanes
    o_chunks = width // 2 // COLS
    kv_core = kv_width // HEAD_DIM
    kv_units = 2 * kv_width // COLS * (width // ROWS)
    units = kv_units + (q_core // COLS) * (width // ROWS) + o_chunks * 2 * q_core // ROWS
    n_slots = units // 2
    bf16, f32 = jnp.bfloat16, jnp.float32
    dma = pltpu.SemaphoreType.DMA
    anywhere = pl.BlockSpec(memory_space=pl.ANY)
    in_vmem = pl.BlockSpec(memory_space=pltpu.VMEM)
    return pl.pallas_call(
        block_kernel,
        name='attend',
        in_specs=[anywhere] * 7,
        out_specs=[in_vmem, in_vmem],
        out_shape=[pltpu.VMEM((chips, width // COLS, tok_chip, COLS), bf16), pltpu.VMEM((table_rows, lanes), f32)],
        scratch_shapes=[
            pltpu.VMEM((n_slots, ROWS, COLS), bf16),
            pltpu.VMEM((tok_chip, width), bf16),
            pltpu.VMEM((chips, 2, tok_chip, kv_width), bf16),
            pltpu.VMEM((heads_core, tok_chip, HEAD_DIM), bf16),
            pltpu.VMEM((2, tok_chip, q_core), bf16),
            pltpu.VMEM((2, table_rows, lanes), f32),
            pltpu.VMEM((chips, table_rows, lanes), f32),
            pltpu.VMEM(ids.shape, ids.dtype),
            pltpu.VMEM(probs.shape, probs.dtype),
            dma((n_slots,)), dma((3,)), dma((2,)), dma((2,)), dma((2, 8)), dma((2, 8)), dma((1, 8)), dma((1, 8)), dma((kv_core,)), dma((kv_core,)),
            dma((o_chunks, 8)), dma((o_chunks, 8)), dma((o_chunks,)), dma((o_chunks,)),
        ],
        compiler_params=pltpu.CompilerParams(collective_id=0, has_side_effects=True, vmem_limit_bytes=63_000_000),
    )(x_loc, w_q, w_k, w_v, w_o, ids, probs)


def solution(mesh):
    group = mesh.shape['sp']
    row_spec = P(('dp', 'sp'), None)
    buf_spec = P(('dp', 'sp'), None, None)

    def device_step(x_loc, w_q, w_k, w_v, w_o, ids_loc, probs_loc):
        h_all, table = attend(x_loc, w_q, w_k, w_v, w_o, ids_loc.T, probs_loc, group)
        buf, hid = build_buffers(h_all, table, x_loc.shape[0], probs_loc.shape[1] // group)
        return hid, buf

    return jax.shard_map(device_step, mesh=mesh, in_specs=(row_spec, P(), P(), P(), P(), row_spec, row_spec), out_specs=(row_spec, buf_spec), check_vma=False)
```

```python
import math
import functools
import jax
import jax.numpy as jnp
from jax import lax
from jax.experimental import pallas as pl
from jax.experimental.pallas import tpu as pltpu
from jax.sharding import PartitionSpec as P

HEAD_DIM = 128
SCORE_SCALE = 1.0 / math.sqrt(HEAD_DIM)
COLS = 256
ROWS = 2048
LAG = 2
Q_STOPS = (5, 7)
CHAIN = 2
GROUP_ROWS = 128
MESH = pl.DeviceIdType.MESH


def route_table(me, ids, probs, seq, table_rows):
    tok_dev, lanes = probs.shape
    per_row = lanes // tok_dev
    sub = lax.broadcasted_iota(jnp.int32, (tok_dev, lanes), 0)
    lane = lax.broadcasted_iota(jnp.int32, (tok_dev, lanes), 1)
    tok = lane - tok_dev * lax.rem(me, per_row)
    diag = tok == sub
    square = lax.broadcasted_iota(jnp.int32, (tok_dev, tok_dev), 0) == lax.broadcasted_iota(jnp.int32, (tok_dev, tok_dev), 1)
    ids = ids.astype(jnp.float32)
    e_sub = [jnp.sum(jnp.where(square, ids[k:k + 1, :], 0.0), axis=1, keepdims=True) for k in range(2)]
    lane_f = lane.astype(jnp.float32)
    p_sub = [jnp.sum(jnp.where(lane_f == e, probs, 0.0), axis=1, keepdims=True) for e in e_sub]
    total = p_sub[0] + p_sub[1]
    to_lanes = lambda col: jnp.sum(jnp.where(diag, col, 0.0), axis=0, keepdims=True)
    e_lane = [to_lanes(e) for e in e_sub]
    valid = jnp.sum(jnp.where(diag, 1.0, 0.0), axis=0, keepdims=True)
    base = (tok_dev * me).astype(jnp.float32)
    dests, gates = [], []
    for k in range(2):
        same = ((e_sub[0] == e_lane[k]) | (e_sub[1] == e_lane[k])) & (sub < tok)
        slot = jnp.sum(jnp.where(same, 1.0, 0.0), axis=0, keepdims=True)
        dests.append(valid * (e_lane[k] * float(seq) + base + slot))
        gates.append(to_lanes(p_sub[k] / total))
    row = lax.broadcasted_iota(jnp.int32, (table_rows, lanes), 0)
    mine = lax.div(me, per_row)
    n_rows = table_rows // 4
    table = jnp.zeros((table_rows, lanes), jnp.float32)
    for n, vec in enumerate(dests + gates):
        table = jnp.where(row == n * n_rows + mine, vec, table)
    return table


def build_kernel(h_ref, table_ref, out_ref, hid_ref, zeros, slots, hid_buf, sems, hid_sem):
    me = lax.axis_index('sp')
    experts_dev, seq, width = out_ref.shape
    n_chips, n_cols, tok_chip, cols = h_ref.shape
    tok_dev = hid_ref.shape[0]
    n_groups = sems.shape[0]
    per_expert = n_groups // experts_dev
    n_rows = table_ref.shape[0] // 4
    lanes = table_ref.shape[1]

    zeros[...] = jnp.zeros_like(zeros)

    table = table_ref[...]
    base = me * experts_dev * seq
    group_first = (base + GROUP_ROWS * lax.broadcasted_iota(jnp.int32, (n_groups, lanes), 0)).astype(jnp.float32)
    hits = jnp.zeros((n_groups, lanes), jnp.float32)
    for r in range(2 * n_rows):
        dest = table[r:r + 1, :]
        hits = jnp.where((dest >= group_first) & (dest < group_first + float(GROUP_ROWS)), 1.0, hits)
    used = jnp.max(hits, axis=1, keepdims=True)
    power = lax.shift_left(jnp.ones((n_groups, 1), jnp.int32), lax.broadcasted_iota(jnp.int32, (n_groups, 1), 0))
    used_bits = jnp.sum(used * power.astype(jnp.float32)).astype(jnp.int32)

    def is_used(n):
        return lax.rem(lax.shift_right_logical(used_bits, n), 2) == 1

    def put(src, n):
        expert, part = lax.div(n, per_expert), lax.rem(n, per_expert)
        at = pl.ds(pl.multiple_of(part * GROUP_ROWS, GROUP_ROWS), GROUP_ROWS)
        return pltpu.make_async_copy(src, out_ref.at[expert, at], sems.at[n])

    def put_zeros(n, carry):
        @pl.when(jnp.logical_not(is_used(n)))
        def _():
            put(zeros, n).start()
        return carry

    lax.fori_loop(0, n_groups, put_zeros, 0)

    per_chip = tok_chip // tok_dev
    chip = lax.div(me, per_chip)
    first = pl.multiple_of(lax.rem(me, per_chip) * tok_dev, tok_dev)
    for n in range(n_cols):
        hid_buf[:, n * cols:(n + 1) * cols] = h_ref[chip, n, pl.ds(first, tok_dev), :]
    hid_copy = pltpu.make_async_copy(hid_buf, hid_ref, hid_sem)
    hid_copy.start()

    spread = lambda n: jnp.concatenate([table[n * n_rows + r:n * n_rows + r + 1, :] for r in range(n_rows)], axis=1)
    dest = [spread(0), spread(1)]
    gate = [spread(2), spread(3)]

    def put_rows(n, carry):
        @pl.when(is_used(n))
        def _():
            row = (lax.broadcasted_iota(jnp.int32, (GROUP_ROWS, seq), 0) + (base + n * GROUP_ROWS)).astype(jnp.float32)
            hit = [dest[0] == row, dest[1] == row]
            gate_row = jnp.sum(jnp.where(hit[0], gate[0], 0.0) + jnp.where(hit[1], gate[1], 0.0), axis=1, keepdims=True)
            pick = jnp.where(hit[0] | hit[1], 1.0, 0.0).astype(jnp.bfloat16)
            for c in range(n_cols):
                rows = h_ref[:, c].reshape(seq, cols)
                got = jnp.dot(pick, rows, preferred_element_type=jnp.float32)
                slots[n, :, c * cols:(c + 1) * cols] = (got * gate_row).astype(jnp.bfloat16)
            put(slots.at[n], n).start()
        return carry

    lax.fori_loop(0, n_groups, put_rows, 0)

    def wait_group(n, carry):
        put(zeros, n).wait()
        return carry

    lax.fori_loop(0, n_groups, wait_group, 0)
    hid_copy.wait()


def build_buffers(h_all, table, tok_dev, experts_dev):
    n_chips, n_cols, tok_chip, cols = h_all.shape
    seq, width = n_chips * tok_chip, n_cols * cols
    n_groups = experts_dev * seq // GROUP_ROWS
    bf16 = jnp.bfloat16
    in_vmem = pl.BlockSpec(memory_space=pltpu.VMEM)
    anywhere = pl.BlockSpec(memory_space=pl.ANY)
    dma = pltpu.SemaphoreType.DMA
    return pl.pallas_call(
        build_kernel,
        name='build_buffers',
        in_specs=[in_vmem, in_vmem],
        out_specs=[anywhere, anywhere],
        out_shape=[jax.ShapeDtypeStruct((experts_dev, seq, width), bf16), jax.ShapeDtypeStruct((tok_dev, width), bf16)],
        scratch_shapes=[
            pltpu.VMEM((GROUP_ROWS, width), bf16), pltpu.VMEM((n_groups, GROUP_ROWS, width), bf16), pltpu.VMEM((tok_dev, width), bf16),
            dma((n_groups,)), dma,
        ],
        compiler_params=pltpu.CompilerParams(vmem_limit_bytes=40 * 1024 * 1024),
        cost_estimate=pl.CostEstimate(flops=2 * experts_dev * seq * seq * width, bytes_accessed=2 * experts_dev * seq * width, transcendentals=0),
    )(h_all, table)


def block_kernel(x_hbm, wq, wk, wv, wo, ids_hbm, probs_hbm, h_all, table_out, wbuf, x_buf, kv, q_buf, o_buf, tab_pair, tabs, ids, probs,
                 w_sem, in_sem, pair_send, pair_recv, kv_send, kv_recv, tab_send, tab_recv, o_send, o_recv, h_send, h_recv, d_send, d_recv):
    tok_dev, width = x_hbm.shape
    chips = kv.shape[0]
    tok_chip = x_buf.shape[0]
    seq = chips * tok_chip
    heads_core = q_buf.shape[0]
    kv_core = kv.shape[3] // HEAD_DIM
    per_kv = heads_core // kv_core
    q_core = heads_core * HEAD_DIM
    out_core = width // 2
    fwd, bwd = chips // 2, chips // 2 - 1
    me = lax.axis_index('sp')
    chip, core = lax.div(me, 2), lax.rem(me, 2)
    other = 1 - core
    partner = {'sp': 2 * chip + other}

    def far(step):
        return {'sp': 2 * lax.rem(chip + chips + step, chips) + core}

    def remote(src, dst, send, recv, device):
        return pltpu.make_async_remote_copy(src_ref=src, dst_ref=dst, send_sem=send, recv_sem=recv, device_id=device, device_id_type=MESH)

    barrier = pltpu.get_barrier_semaphore()
    near = [partner, far(1), far(-1), far(2), far(-2)]
    for device in near:
        pl.semaphore_signal(barrier, inc=1, device_id=device, device_id_type=MESH)

    n_slots = wbuf.shape[0]
    kv_units = 2 * (kv.shape[3] // COLS) * (width // ROWS)
    half_units = q_core // ROWS
    chunk_units = 2 * half_units
    in_units = width // ROWS
    q_chunks = q_core // COLS
    o_chunks = out_core // COLS
    kv_chunks = kv.shape[3] // COLS

    def load(src, row, col, slot):
        return pltpu.make_async_copy(src.at[pl.ds(row, ROWS), pl.ds(pl.multiple_of(col, COLS), COLS)], wbuf.at[slot], w_sem.at[slot])

    def wait_unit(slot):
        load(wk, 0, 0, slot).wait()

    def start_q(n):
        for r in range(in_units):
            load(wq, r * ROWS, core * q_core + n * COLS, lax.rem(kv_units + in_units * n + r, n_slots)).start()

    first_o = kv_units + in_units * q_chunks - n_slots

    def start_o(k):
        j, r = lax.div(k, chunk_units), lax.rem(k, chunk_units)
        half = jnp.where(r < half_units, core, other)
        row = pl.multiple_of(half * q_core + lax.rem(r, half_units) * ROWS, ROWS)
        load(wo, row, core * out_core + j * COLS, first_o + k).start()

    own = pl.ds(pl.multiple_of(core * tok_dev, tok_dev), tok_dev)
    theirs = pl.ds(pl.multiple_of(other * tok_dev, tok_dev), tok_dev)
    x_in = pltpu.make_async_copy(x_hbm, x_buf.at[own], in_sem.at[0])
    x_in.start()
    x_in.wait()
    slot = 0
    for src in (wk, wv):
        for n in range(kv_chunks):
            for r in range(in_units):
                load(src, r * ROWS, core * kv.shape[3] + n * COLS, slot).start()
                slot += 1
    ids_in = pltpu.make_async_copy(ids_hbm, ids, in_sem.at[1])
    probs_in = pltpu.make_async_copy(probs_hbm, probs, in_sem.at[2])
    ids_in.start()
    probs_in.start()
    pl.semaphore_wait(barrier, len(near))

    x_pair = remote(x_buf.at[own], x_buf.at[own], pair_send.at[0], pair_recv.at[0], partner)
    x_pair.start()
    q_first = (n_slots - kv_units) // in_units
    lax.fori_loop(0, q_first, lambda n, c: (start_q(n), c)[1], 0)
    remote(x_buf.at[theirs], x_buf.at[theirs], pair_send.at[0], pair_recv.at[0], partner).wait_recv()

    def wait_units(first, count):
        for r in range(count):
            wait_unit(first + r)

    def project(pair_slot):
        w = wbuf[pl.ds(pair_slot, in_units)].reshape(width, COLS)
        return jnp.dot(x_buf[...], w, preferred_element_type=jnp.float32).astype(jnp.bfloat16)

    def two_step(piece, sends, recvs, n, source, reach, step, back):
        block = lax.rem(chip + source, chips) if back else lax.rem(chip + chips - source, chips)
        part = piece(block, n)
        if reach == fwd:
            part = part.at[pl.ds(back * tok_dev, tok_dev)]
        at = 4 * back + reach - 1
        return remote(part, part, sends.at[n, at], recvs.at[n, at], far(-step) if back else far(step))

    def two_step_start(*args):
        for reach in (1, 2):
            for back in range(2):
                two_step(*args, 0, reach, reach, back).start()

    def two_step_onward(*args):
        for back in range(2):
            two_step(*args, 2, 2, 2, back).wait_recv()
            for reach in range(3, fwd + 1):
                two_step(*args, 2, reach, reach - 2, back).start()
        for back in range(2):
            two_step(*args, 1, 1, 1, back).wait_recv()

    def two_step_last(*args):
        for reach in range(3, fwd + 1):
            for back in range(2):
                two_step(*args, reach, reach, 1, back).wait_recv()

    def two_step_sent(*args):
        for back in range(2):
            for reach in range(1, fwd + 1):
                two_step(*args, 0 if reach < 3 else 2, reach, 1, back).wait_send()

    def kv_piece(block, which):
        return kv.at[block, which]

    def h_piece(block, j):
        return h_all.at[block, core * o_chunks + j]

    def tab_piece(block, which):
        return tabs.at[block]

    def ring(piece, sends, recvs, which, s, back, arriving=0):
        s_at = s + arriving
        block = lax.rem(chip + s_at, chips) if back else lax.rem(chip + chips - s_at, chips)
        part = piece(block, which)
        return remote(part, part, sends.at[which, 4 * back + s], recvs.at[which, 4 * back + s], far(-1) if back else far(1))

    def ring_start(*args):
        ring(*args, 0, 0).start()
        ring(*args, 0, 1).start()

    def ring_hop(*args):
        *args, s = args
        ring(*args, s, 0, 1).wait_recv()
        if s + 1 < fwd:
            ring(*args, s + 1, 0).start()
        if s < bwd:
            ring(*args, s, 1, 1).wait_recv()
            if s + 1 < bwd:
                ring(*args, s + 1, 1).start()

    kv_ring = (kv_piece, kv_send, kv_recv)
    tab_ring = (tab_piece, tab_send, tab_recv)

    slot = 0
    for which in range(2):
        for n in range(kv_chunks):
            wait_units(slot, in_units)
            kv[chip, which, :, n * COLS:(n + 1) * COLS] = project(slot)
            slot += in_units
        two_step_start(*kv_ring, which)

    for n in range(q_first, q_chunks):
        start_q(n)
    early = kv_units - first_o
    for k in range(early):
        start_o(k)

    ids_in.wait()
    probs_in.wait()
    tab_pair[0] = route_table(me, ids[...], probs[...], seq, tab_pair.shape[1])
    t_pair = remote(tab_pair.at[0], tab_pair.at[1], pair_send.at[1], pair_recv.at[1], partner)
    t_pair.start()

    heads_chunk = COLS // HEAD_DIM

    def q_step(m, carry):
        first = lax.rem(kv_units + 2 * in_units * m, n_slots)
        wait_units(first, 2 * in_units)
        for half in range(2):
            res = project(first + in_units * half)
            for i in range(heads_chunk):
                q_buf[heads_chunk * (2 * m + half) + i] = res[:, i * HEAD_DIM:(i + 1) * HEAD_DIM]

        @pl.when(2 * m < q_first)
        def _():
            for r in range(2 * in_units):
                start_o(early + 2 * in_units * m + r)
        return carry

    lax.fori_loop(0, Q_STOPS[0], q_step, 0)
    t_pair.wait_recv()
    tabs[chip] = tab_pair[0] + tab_pair[1]
    ring_start(*tab_ring, 0)
    two_step_onward(*kv_ring, 0)
    lax.fori_loop(Q_STOPS[0], Q_STOPS[1], q_step, 0)
    two_step_onward(*kv_ring, 1)
    lax.fori_loop(Q_STOPS[1], q_chunks // 2, q_step, 0)
    ring_hop(*tab_ring, 0, 0)
    for which in range(2):
        two_step_last(*kv_ring, which)

    rows = per_kv * tok_chip
    q_pos = tok_chip * chip + lax.rem(lax.broadcasted_iota(jnp.int32, (rows, seq), 0), tok_chip)
    seen = lax.broadcasted_iota(jnp.int32, (rows, seq), 1) <= q_pos
    o_copies = []
    for g in range(kv_core):
        lanes = slice(g * HEAD_DIM, (g + 1) * HEAD_DIM)
        qg = q_buf[g * per_kv:(g + 1) * per_kv].reshape(rows, HEAD_DIM)
        kg = kv[:, 0, :, lanes].reshape(seq, HEAD_DIM)
        vg = kv[:, 1, :, lanes].reshape(seq, HEAD_DIM)
        s = lax.dot_general(qg, kg, (((1,), (1,)), ((), ())), preferred_element_type=jnp.float32) * SCORE_SCALE
        s = jnp.where(seen, s, -1e30)
        p = jnp.exp(s - jnp.max(s, axis=1, keepdims=True))
        p = (p / jnp.sum(p, axis=1, keepdims=True)).astype(jnp.bfloat16)
        o = jnp.dot(p, vg, preferred_element_type=jnp.float32).astype(jnp.bfloat16)
        for h in range(per_kv):
            col = (g * per_kv + h) * HEAD_DIM
            o_buf[0, :, col:col + HEAD_DIM] = o[h * tok_chip:(h + 1) * tok_chip]
        span = pl.ds(g * per_kv * HEAD_DIM, per_kv * HEAD_DIM)
        copy = remote(o_buf.at[0, :, span], o_buf.at[1, :, span], o_send.at[g], o_recv.at[g], partner)
        copy.start()
        o_copies.append(copy)
    ring_hop(*tab_ring, 0, 1)

    h_ring = (h_piece, h_send, h_recv)

    def chain_hop(j, reach):
        for back in range(2):
            two_step(*h_ring, j, reach, reach, 1, back).wait_recv()
            if reach < fwd:
                two_step(*h_ring, j, reach, reach + 1, 1, back).start()
        if reach == fwd:
            h_pair(j, core).start()

    def last_step(j):
        two_step_last(*h_ring, j)
        h_pair(j, core).start()

    def h_pair(j, half):
        cols = h_all.at[:, half * o_chunks + j]
        return remote(cols, cols, d_send.at[j], d_recv.at[j], partner)

    def o_step(j, carry):
        at = first_o + chunk_units * j

        @pl.when(j == 0)
        def _():
            for copy in o_copies:
                copy.wait_recv()
        wait_units(at, chunk_units)
        acc = jnp.dot(o_buf[0], wbuf[pl.ds(at, half_units)].reshape(q_core, COLS), preferred_element_type=jnp.float32)
        acc += jnp.dot(o_buf[1], wbuf[pl.ds(at + half_units, half_units)].reshape(q_core, COLS), preferred_element_type=jnp.float32)
        x_cols = x_buf[:, pl.ds(pl.multiple_of(core * out_core + j * COLS, COLS), COLS)]
        h_all[chip, core * o_chunks + j] = (x_cols.astype(jnp.float32) + acc).astype(jnp.bfloat16)
        for back in range(2):
            two_step(*h_ring, j, 0, 1, 1, back).start()

        @pl.when(j >= CHAIN)
        def _():
            for back in range(2):
                two_step(*h_ring, j, 0, 2, 2, back).start()

        for reach in range(1, fwd):
            late = j - LAG * reach

            @pl.when((late >= 0) & (late < CHAIN))
            def _(late=late, reach=reach):
                chain_hop(late, reach)

        @pl.when(j == 3)
        def _():
            ring_hop(*tab_ring, 0, 2)

        @pl.when(j >= CHAIN + LAG)
        def _():
            two_step_onward(*h_ring, j - LAG)

        @pl.when(j >= CHAIN + 2 * LAG)
        def _():
            last_step(j - 2 * LAG)
        return carry

    lax.fori_loop(0, o_chunks, o_step, 0)
    for reach in range(1, fwd):
        for j in range(max(0, o_chunks - LAG * reach), CHAIN):
            chain_hop(j, reach)
    for j in range(o_chunks - LAG, o_chunks):
        two_step_onward(*h_ring, j)
    ring_hop(*tab_ring, 0, fwd - 1)
    table_out[...] = jnp.sum(tabs[...], axis=0)
    for j in range(CHAIN):
        chain_hop(j, fwd)
    for j in range(max(CHAIN, o_chunks - 2 * LAG), o_chunks - 1):
        last_step(j)
    x_pair.wait_send()
    t_pair.wait_send()
    for back, hops in ((0, fwd), (1, bwd)):
        for n in range(hops):
            ring(*tab_ring, 0, n, back).wait_send()
    for which in range(2):
        two_step_sent(*kv_ring, which)
    for copy in o_copies:
        copy.wait_send()
    lax.fori_loop(0, o_chunks - 1, lambda n, c: (two_step_sent(*h_ring, n), c)[1], 0)
    last_step(o_chunks - 1)
    for j in range(o_chunks):
        h_pair(j, other).wait_recv()

    for n in range(o_chunks - 1, o_chunks):
        two_step_sent(*h_ring, n)
    for n in range(o_chunks):
        h_pair(n, core).wait_send()


def attend(x_loc, w_q, w_k, w_v, w_o, ids, probs, group):
    tok_dev, width = x_loc.shape
    chips = group // 2
    tok_chip = 2 * tok_dev
    heads_core = w_q.shape[1] // HEAD_DIM // 2
    kv_width = w_k.shape[1] // 2
    q_core = heads_core * HEAD_DIM
    lanes = probs.shape[1]
    table_rows = 4 * chips * tok_chip // lanes
    o_chunks = width // 2 // COLS
    kv_core = kv_width // HEAD_DIM
    kv_units = 2 * kv_width // COLS * (width // ROWS)
    units = kv_units + (q_core // COLS) * (width // ROWS) + o_chunks * 2 * q_core // ROWS
    n_slots = units // 2
    bf16, f32 = jnp.bfloat16, jnp.float32
    dma = pltpu.SemaphoreType.DMA
    anywhere = pl.BlockSpec(memory_space=pl.ANY)
    in_vmem = pl.BlockSpec(memory_space=pltpu.VMEM)
    return pl.pallas_call(
        block_kernel,
        name='attend',
        in_specs=[anywhere] * 7,
        out_specs=[in_vmem, in_vmem],
        out_shape=[pltpu.VMEM((chips, width // COLS, tok_chip, COLS), bf16), pltpu.VMEM((table_rows, lanes), f32)],
        scratch_shapes=[
            pltpu.VMEM((n_slots, ROWS, COLS), bf16),
            pltpu.VMEM((tok_chip, width), bf16),
            pltpu.VMEM((chips, 2, tok_chip, kv_width), bf16),
            pltpu.VMEM((heads_core, tok_chip, HEAD_DIM), bf16),
            pltpu.VMEM((2, tok_chip, q_core), bf16),
            pltpu.VMEM((2, table_rows, lanes), f32),
            pltpu.VMEM((chips, table_rows, lanes), f32),
            pltpu.VMEM(ids.shape, ids.dtype),
            pltpu.VMEM(probs.shape, probs.dtype),
            dma((n_slots,)), dma((3,)), dma((2,)), dma((2,)), dma((2, 8)), dma((2, 8)), dma((1, 8)), dma((1, 8)), dma((kv_core,)), dma((kv_core,)),
            dma((o_chunks, 8)), dma((o_chunks, 8)), dma((o_chunks,)), dma((o_chunks,)),
        ],
        compiler_params=pltpu.CompilerParams(collective_id=0, has_side_effects=True, vmem_limit_bytes=63_000_000),
    )(x_loc, w_q, w_k, w_v, w_o, ids, probs)


def solution(mesh):
    group = mesh.shape['sp']
    row_spec = P(('dp', 'sp'), None)
    buf_spec = P(('dp', 'sp'), None, None)

    def device_step(x_loc, w_q, w_k, w_v, w_o, ids_loc, probs_loc):
        h_all, table = attend(x_loc, w_q, w_k, w_v, w_o, ids_loc.T, probs_loc, group)
        buf, hid = build_buffers(h_all, table, x_loc.shape[0], probs_loc.shape[1] // group)
        return hid, buf

    return jax.shard_map(device_step, mesh=mesh, in_specs=(row_spec, P(), P(), P(), P(), row_spec, row_spec), out_specs=(row_spec, buf_spec), check_vma=False)
```
